8 devices in a mesh: batch: 1 (over z), col: 2 (over y), row: 4 (over x, core).
Axes of the slice: x: 2, y: 2, z: 1, core: 2. Of those that a mesh axis runs over, the one named last changes fastest.
Arguments:
- lower_cyc: float32 [3072, 3072], P(('batch', 'row'), 'col')
Outputs:
- output: float32 [3072, 3072], P(('batch', 'row'), 'col')
All inputs are finite; a program needn't handle non-finite values.
Results may differ from the reference program's by a relative error of at most 0.001.
Values sent between devices are 32-bit elements.
A program may use at most 1 GiB of HBM per device.

```python
import jax
import jax.numpy as jnp
from jax import lax

N = 3072
DEPTH = 3
BLK = 8
PX = 4
PY = 2


def to_cyclic(matrix):
    blocks6 = matrix.reshape(N // (PX * BLK), PX, BLK, N // (PY * BLK), PY, BLK)
    return blocks6.transpose(1, 0, 2, 4, 3, 5).reshape(N, N)


def to_natural(cyclic):
    blocks6 = cyclic.reshape(PX, N // (PX * BLK), BLK, PY, N // (PY * BLK), BLK)
    return blocks6.transpose(1, 0, 2, 4, 3, 5).reshape(N, N)


def setup_inputs(seed: int = 0, part: int = 0) -> dict:
    base_key = jax.random.fold_in(jax.random.key(seed), part)
    key_diag, key_low = jax.random.split(base_key)
    diag_vals = jax.random.uniform(key_diag, (N,), jnp.float32, 2.0, 4.0)
    low_vals = jax.random.normal(key_low, (N, N), jnp.float32) * (2.0 / N ** 0.5)
    row_ids = jnp.arange(N)[:, None]
    col_ids = jnp.arange(N)[None, :]
    natural = jnp.where(row_ids > col_ids, low_vals, 0.0) + jnp.where(row_ids == col_ids, diag_vals[:, None], 0.0)
    return {"lower_cyc": to_cyclic(natural)}


def highest_dot(left, right):
    return jnp.dot(left, right, precision=lax.Precision.HIGHEST, preferred_element_type=jnp.float32)


def invert_block(mat_block, levels_left):
    block_size = mat_block.shape[0]
    if levels_left == 0:
        identity = jnp.eye(block_size, dtype=jnp.float32)
        return lax.linalg.triangular_solve(mat_block, identity, left_side=True, lower=True)
    half_size = block_size // 2
    inv_upper = invert_block(mat_block[:half_size, :half_size], levels_left - 1)
    inv_lower = invert_block(mat_block[half_size:, half_size:], levels_left - 1)
    temp_prod = highest_dot(mat_block[half_size:, :half_size], inv_upper)
    off_diag = -highest_dot(inv_lower, temp_prod)
    zero_block = jnp.zeros((half_size, half_size), jnp.float32)
    upper_rows = jnp.concatenate([inv_upper, zero_block], axis=1)
    lower_rows = jnp.concatenate([off_diag, inv_lower], axis=1)
    return jnp.concatenate([upper_rows, lower_rows], axis=0)


def reference(lower_cyc):
    return to_cyclic(invert_block(to_natural(lower_cyc), DEPTH))
```

```python
import functools

import jax
import jax.numpy as jnp
from jax import lax
from jax.experimental import pallas as pl
from jax.experimental.pallas import tpu as pltpu
from jax.sharding import PartitionSpec as P

MESH = pl.DeviceIdType.MESH
F32 = jnp.float32

DIAG = [(i, i) for i in range(12)]
OFF_A = [(i, j) for i in range(1, 6) for j in range(i)]
OFF_B = [(i + 6, j + 6) for i in range(1, 6) for j in range(i)]
TILES = DIAG + OFF_A + OFF_B
TIDX = {ij: t for t, ij in enumerate(TILES)}
CHUNKS = [(0, 6), (6, 12), (12, 18), (18, 22), (22, 27), (27, 33), (33, 37), (37, 42)]
NC = len(CHUNKS)
NF, NG, ND, SO, SF, SG, SD = range(7)
W, T2, JW, HW = 128, 256, 384, 768


def dot(a, b):
    return jnp.dot(a, b, precision=lax.Precision.HIGHEST, preferred_element_type=F32)


def kernel(l_hbm, out, lt, c0, xa, xb, bx, tt, db, oa, xc, oc, zz, acc, ys,
           loc, snd, rcv, csnd, crcv, tsnd, trcv, osnd, orcv, misc_s, misc_r, osem, bar_dummy):
    del bar_dummy
    row = lax.axis_index("row")
    y = lax.axis_index("col")
    x = row // 2
    k = row % 2
    ox, ok, oy = 1 - x, 1 - k, 1 - y
    fid = {"row": row + (1 - k) * 2 * (1 - 2 * x), "col": y + k * (1 - 2 * y)}
    gid = {"row": row + k * 2 * (1 - 2 * x), "col": y + (1 - k) * (1 - 2 * y)}
    sid = {"row": 2 * x + ok, "col": y}
    xid = {"row": 2 * ox + k, "col": y}
    yid = {"row": row, "col": oy}
    fx, fy = x + (1 - k) * (1 - 2 * x), y + k * (1 - 2 * y)
    gx, gy = x + k * (1 - 2 * x), y + (1 - k) * (1 - 2 * y)

    started = []

    def remote(src, dst, ss, rs, dev):
        cp = pltpu.make_async_remote_copy(src_ref=src, dst_ref=dst, send_sem=ss, recv_sem=rs,
                                          device_id=dev, device_id_type=MESH)
        return cp

    def piece(c, q, p, xs):
        a, b = CHUNKS[c]
        return lt.at[a:b, q, p, :, xs, :, :]

    def put(c, kind, q, xs, dev):
        ref = piece(c, q, k, xs)
        cp = remote(ref, ref, snd.at[c, kind], rcv.at[c, kind], dev)
        cp.start()
        started.append(cp)

    def got(c, kind, q, p, xs):
        ref = piece(c, q, p, xs)
        remote(ref, ref, snd.at[c, kind], rcv.at[c, kind], sid).wait_recv()

    def local_copies(c):
        a, b = CHUNKS[c]
        return [pltpu.make_async_copy(l_hbm.at[8 * i:8 * i + 8, :, W * j:W * j + W],
                                      lt.at[a + n, y, k, :, x, :, :], loc.at[a + n])
                for n, (i, j) in enumerate(TILES[a:b])]

    for c in range(NC):
        for cp in local_copies(c):
            cp.start()
    c0own = c0.at[y, k]
    c0load = pltpu.make_async_copy(l_hbm.at[48:96, :, 0:HW], c0own, loc.at[42])
    c0load.start()

    barrier = pltpu.get_barrier_semaphore()
    for dev in (fid, gid, sid):
        pl.semaphore_signal(barrier, inc=1, device_id=dev, device_id_type=MESH)
    pl.semaphore_wait(barrier, 3)

    for c in range(NC):
        for cp in local_copies(c):
            cp.wait()
        put(c, NF, y, x, fid)
        if c < 2:
            put(c, NG, y, x, gid)
        put(c, SO, y, x, sid)

    c0load.wait()

    def cref(s, q, p):
        return c0.at[q, p, pl.ds(8 * s, 8)]

    def cput(s, kind, q, dev):
        ref = cref(s, q, k)
        return remote(ref, ref, csnd.at[s, kind], crcv.at[s, kind], dev)

    for s in range(6):
        cput(s, 1, y, sid).start()

    xa[...] = jnp.zeros(xa.shape, F32)
    xb[...] = jnp.zeros(xb.shape, F32)
    zz[...] = jnp.zeros(zz.shape, F32)

    def serve_f(c):
        got(c, NF, fy, k, fx)
        put(c, ND, fy, fx, gid)
        put(c, SF, fy, fx, sid)
        if c + 2 < NC:
            put(c + 2, NG, y, x, gid)

    def serve_g(c):
        got(c, NG, gy, k, gx)
        put(c, SG, gy, gx, sid)
        got(c, ND, oy, k, ox)
        put(c, SD, oy, ox, sid)

    def ready(c):
        got(c, SO, y, ok, x)
        got(c, SF, gy, ok, gx)
        got(c, SG, fy, ok, fx)
        got(c, SD, oy, ok, ox)

    serve_f(0)
    serve_f(1)
    serve_g(0)
    serve_g(1)
    serve_f(2)
    ready(0)
    ready(1)
    serve_f(3)

    lane = lax.broadcasted_iota(jnp.int32, (8, W), 1)
    grp = lane // 16
    G6 = 6
    sub = {}
    for p in range(2):
        for sg in range(2):
            for q in range(2):
                rows = []
                for g in range(G6):
                    v = jnp.zeros((8, W), F32)
                    for m in range(8):
                        v = jnp.where(grp == m, lt[2 * g + k, q, p, m, sg], v)
                    rows.append(v)
                sub[2 * sg + p, q] = jnp.concatenate(rows, axis=0)
    lane48 = lax.broadcasted_iota(jnp.int32, (8 * G6, W), 1)
    sub48 = lax.broadcasted_iota(jnp.int32, (8 * G6, W), 0) % 8
    base48 = (lane48 // 16) * 16
    yv = {}
    for be in range(4):
        for q in range(2):
            if be % 2 == q:
                yv[be, q] = jnp.where(lane48 % 16 == 8 * (be // 2) + sub48, 1.0, 0.0).astype(F32)
            else:
                yv[be, q] = jnp.zeros((8 * G6, W), F32)

    def rowcast(v, e):
        v3 = v.reshape(G6, 8, W)[:, e:e + 1, :]
        return jnp.broadcast_to(v3, (G6, 8, W)).reshape(8 * G6, W)

    for be in range(4):
        for e in range(8):
            idx = base48 + (8 * (be // 2) + e)
            gs = {b2: jnp.take_along_axis(sub[b2, be % 2], idx, axis=1, mode="promise_in_bounds")
                  for b2 in range(be, 4)}
            rinv = 1.0 / rowcast(gs[be], e)
            for q in range(2):
                piv = rowcast(yv[be, q], e) * rinv
                for b2 in range(be, 4):
                    new = yv[b2, q] - gs[b2] * piv
                    if b2 == be:
                        new = jnp.where(sub48 > e, new, jnp.where(sub48 == e, piv, yv[b2, q]))
                    yv[b2, q] = new
    for be in range(4):
        for q in range(2):
            ys[be, q] = yv[be, q].reshape(G6, 8, W)

    lane256 = lax.broadcasted_iota(jnp.int32, (8, T2), 1) % W

    def invert_some(g0, count):
        dd, ll = [], []
        for n in range(count):
            g = g0 + n
            rows = []
            for p in range(2):
                for m in range(8):
                    for sg in range(2):
                        parts = [jnp.where(grp == m, ys[2 * sg + p, q, g], 0.0) for q in range(2)]
                        rows.append(jnp.concatenate(parts, axis=1))
            dd.append(rows)
            ll.append([jnp.concatenate([lt[2 * g + k, q, p, m, sg] for q in range(2)], axis=1)
                       for p in range(2) for m in range(8) for sg in range(2)])
        for h8 in (2, 4, 8):
            odd = [b for b in range(32) if (b % 16) // h8 % 2 == 1]
            zero = jnp.zeros((8, T2), F32)
            tds = []
            for n in range(count):
                mo = [jnp.where(lane256 // (8 * h8) == (b % 16) // h8 - 1, ll[n][b], 0.0) for b in odd]
                tds.append(dot(jnp.concatenate(mo, axis=0), jnp.concatenate(dd[n], axis=0)))
            for n in range(count):
                tfull = [zero] * 32
                for o, b in enumerate(odd):
                    tfull[b] = tds[n][8 * o:8 * o + 8]
                xo = dot(jnp.concatenate([dd[n][b] for b in odd], axis=0), jnp.concatenate(tfull, axis=0))
                for o, b in enumerate(odd):
                    dd[n][b] = dd[n][b] - xo[8 * o:8 * o + 8]
        for n in range(count):
            db[g0 + n, k] = jnp.concatenate(dd[n], axis=0)

    def inv_body(it, carry):
        invert_some(3 * it, 3)
        return carry

    lax.fori_loop(0, 2, inv_body, 0)
    dbcopy = remote(db.at[:, k], db.at[:, k], misc_s.at[0], misc_r.at[0], sid)
    dbcopy.start()

    serve_f(4)
    serve_f(5)
    serve_g(2)
    ready(2)
    remote(db.at[:, ok], db.at[:, ok], misc_s.at[0], misc_r.at[0], sid).wait_recv()

    def ltile(t):
        return jnp.concatenate([lt[t, q].reshape(T2, W) for q in range(2)], axis=1)

    need = [0, 1, 1, 0, 0, 1]

    def place_a(i):
        @pl.when(k == need[i])
        def _():
            t = i // 2
            d = db[i // 2, i % 2, :, pl.ds(pl.multiple_of(y * W, W), W)]
            xa[i, :, :, :, :, W * t:W * t + W] = d.reshape(2, 8, 2, 8, W)

    def step_a(i):
        for j in range(i):
            n = W * (j // 2 + 1)
            d = dot(ltile(TIDX[i, j]), xa[j, :, :, :, :, 0:n].reshape(T2, n))
            n0 = 0 if j == 0 else W * ((j - 1) // 2 + 1)
            if n0:
                acc[:, 0:n0] = acc[:, 0:n0] + d[:, 0:n0]
            if n > n0:
                acc[:, n0:n] = d[:, n0:n]
        n = W * ((i + 1) // 2)
        r = -dot(db[i // 2, i % 2], acc[:, 0:n])
        xa[i, :, :, :, :, 0:n] = r.reshape(2, 8, 2, 8, n)
        place_a(i)

    def place_b(i):
        d = db[3 + i // 2, i % 2, :, pl.ds(pl.multiple_of(k * W, W), W)]
        xb[i, :, :, :, :, W * i:W * i + W] = d.reshape(2, 8, 2, 8, W)

    def step_b(i):
        for j in range(i):
            n = W * (j + 1)
            d = dot(ltile(TIDX[i + 6, j + 6]), xb[j, :, :, :, :, 0:n].reshape(T2, n))
            if j:
                acc[:, 0:n - W] = acc[:, 0:n - W] + d[:, 0:n - W]
            acc[:, n - W:n] = d[:, n - W:n]
        n = W * i
        r = -dot(db[3 + i // 2, i % 2], acc[:, 0:n])
        xb[i, :, :, :, :, 0:n] = r.reshape(2, 8, 2, 8, n)
        place_b(i)

    place_a(0)
    for i in (1, 2, 3):
        step_a(i)
    serve_f(6)
    serve_f(7)
    for s in range(6):
        cput(s, 0, y, yid).start()
    serve_g(3)
    ready(3)
    step_a(4)
    serve_g(4)
    ready(4)
    step_a(5)

    oacopy = remote(xa.at[:, ok, :, x, :, :], oa, misc_s.at[1], misc_r.at[1], sid)
    oacopy.start()

    outs = []

    def put_out(src, dst):
        cp = pltpu.make_async_copy(src, dst, osem.at[len(outs)])
        cp.start()
        outs.append(cp)

    def jcol(t, kk):
        return [kk, 3 - kk, 4 + kk][t]

    def lanes(t, kk):
        return pl.ds(pl.multiple_of(W * jcol(t, kk), W), W)

    for i in range(6):
        put_out(zz, out.at[i, :, :, HW:1536])
    for t in range(3):
        put_out(xa.at[:, k, :, x, :, W * t:W * t + W], out.at[0:6, :, :, lanes(t, k)])

    serve_g(5)
    ready(5)
    place_b(0)
    for i in (1, 2, 3):
        step_b(i)
    serve_g(6)
    ready(6)
    step_b(4)
    serve_g(7)
    ready(7)
    step_b(5)

    bxcopy = remote(xb.at[:, :, :, x, :, :], bx.at[k], misc_s.at[2], misc_r.at[2], sid)
    bxcopy.start()
    bxlocal = pltpu.make_async_copy(xb.at[:, :, :, x, :, :], bx.at[k], loc.at[43])
    bxlocal.start()

    def tput(s):
        ref = tt.at[s, :, :, x, :, :]
        return remote(ref, ref, tsnd.at[s], trcv.at[s], xid)

    def do_t(s):
        cput(s, 0, oy, yid).wait_recv()
        cput(s, 2, oy, sid).start()
        remote(cref(s, y, ok), cref(s, y, ok), csnd.at[s, 1], crcv.at[s, 1], sid).wait_recv()
        remote(cref(s, oy, ok), cref(s, oy, ok), csnd.at[s, 2], crcv.at[s, 2], sid).wait_recv()
        for u in range(3):
            n = W * (u + 1)
            parts = []
            for j in (2 * u, 2 * u + 1):
                for q in range(2):
                    parts.append(c0[q, :, pl.ds(8 * s, 8), :, W * j:W * j + W].reshape(W, W))
            rhs = jnp.concatenate([xa[2 * u + e, :, :, :, :, 0:n].reshape(T2, n) for e in range(2)], axis=0)
            d = dot(jnp.concatenate(parts, axis=1), rhs)
            if u:
                acc[0:W, 0:n - W] = acc[0:W, 0:n - W] + d[:, 0:n - W]
            acc[0:W, n - W:n] = d[:, n - W:n]
        tt[s, :, :, x, :, :] = acc[0:W, 0:JW].reshape(2, 8, 8, JW)
        tput(s).start()

    def do_x(s):
        ref = tt.at[s, :, :, ox, :, :]
        remote(ref, ref, tsnd.at[s], trcv.at[s], xid).wait_recv()
        acc[W:T2, 0:JW] = jnp.zeros((W, JW), F32)

        def body(u, carry):
            ln = pl.ds(pl.multiple_of(u * W, W), W)
            lhs = jnp.concatenate([bx[q, s, :, :, :, ln].reshape(W, W) for q in range(2)], axis=1)
            acc[W:T2, 0:JW] = acc[W:T2, 0:JW] - dot(lhs, tt[u].reshape(T2, JW))
            return carry

        lax.fori_loop(0, s + 1, body, 0)
        xc[s] = acc[W:T2, 0:JW].reshape(2, 8, 8, JW)
        remote(xc.at[s, ok], oc.at[s], osnd.at[s], orcv.at[s], sid).start()
        for t in range(3):
            put_out(xc.at[s, k, :, :, W * t:W * t + W], out.at[6 + s, :, :, lanes(t, k)])

    for s in range(8):
        if s < 6:
            do_t(s)
        if s == 1:
            bxlocal.wait()
            remote(bx.at[ok], bx.at[ok], misc_s.at[2], misc_r.at[2], sid).wait_recv()
            put_out(bx.at[y, :, k], out.at[6:12, :, :, HW:1536])
            remote(oa, oa, misc_s.at[1], misc_r.at[1], sid).wait_recv()
            for t in range(3):
                put_out(oa.at[:, :, :, W * t:W * t + W], out.at[0:6, :, :, lanes(t, ok)])
        if s >= 2:
            do_x(s - 2)
    for s in range(6):
        remote(oc.at[s], oc.at[s], osnd.at[s], orcv.at[s], sid).wait_recv()
        for t in range(3):
            put_out(oc.at[s, :, :, W * t:W * t + W], out.at[6 + s, :, :, lanes(t, ok)])

    for cp in started:
        cp.wait_send()
    for s in range(6):
        cput(s, 0, y, yid).wait_send()
        cput(s, 1, y, sid).wait_send()
        cput(s, 2, oy, sid).wait_send()
        tput(s).wait_send()
        remote(xc.at[s, ok], oc.at[s], osnd.at[s], orcv.at[s], sid).wait_send()
    dbcopy.wait_send()
    oacopy.wait_send()
    bxcopy.wait_send()
    for cp in outs:
        cp.wait()


def solution(mesh):
    spec = P(("batch", "row"), "col")
    vm = lambda *shape: pltpu.VMEM(shape, F32)
    dma = lambda *shape: pltpu.SemaphoreType.DMA(shape)

    def body(local_l):
        got = pl.pallas_call(
            kernel,
            name="tri_inverse",
            out_shape=jax.ShapeDtypeStruct((12, 8, 8, 1536), F32),
            in_specs=[pl.BlockSpec(memory_space=pl.ANY)],
            out_specs=pl.BlockSpec(memory_space=pl.ANY),
            scratch_shapes=[
                vm(42, 2, 2, 8, 2, 8, W),
                vm(2, 2, 48, 8, HW),
                vm(6, 2, 8, 2, 8, JW),
                vm(6, 2, 8, 2, 8, HW),
                vm(2, 6, 2, 8, 8, HW),
                vm(6, 2, 8, 2, 8, JW),
                vm(6, 2, T2, T2),
                vm(6, 8, 8, JW),
                vm(6, 2, 8, 8, JW),
                vm(6, 8, 8, JW),
                vm(8, 8, HW),
                vm(T2, HW),
                vm(4, 2, 6, 8, W),
                dma(44), dma(NC, 7), dma(NC, 7), dma(6, 3), dma(6, 3), dma(6), dma(6),
                dma(6), dma(6), dma(3), dma(3), dma(64), pltpu.SemaphoreType.REGULAR,
            ],
            compiler_params=pltpu.CompilerParams(
                collective_id=0, has_side_effects=True, vmem_limit_bytes=60 * 2**20),
        )(local_l.reshape(96, 8, 1536))
        return got.reshape(HW, 1536)

    return jax.shard_map(body, mesh=mesh, in_specs=(spec,), out_specs=spec, check_vma=False)
```

```python
import functools

import jax
import jax.numpy as jnp
from jax import lax
from jax.experimental import pallas as pl
from jax.experimental.pallas import tpu as pltpu
from jax.sharding import PartitionSpec as P

MESH = pl.DeviceIdType.MESH
F32 = jnp.float32

DIAG = [(i, i) for i in range(12)]
OFF_A = [(i, j) for i in range(1, 6) for j in range(i)]
OFF_B = [(i + 6, j + 6) for i in range(1, 6) for j in range(i)]
TILES = DIAG[:6] + OFF_A + DIAG[6:] + OFF_B
TIDX = {ij: t for t, ij in enumerate(TILES)}
CHUNKS = [(0, 6), (6, 12), (12, 16), (16, 21), (21, 27), (27, 33), (33, 37), (37, 42)]
NC = len(CHUNKS)
NF, NG, ND, SO, SF, SG, SD = range(7)
CP = [(0, 0, 8), (1, 0, 8), (2, 0, 8), (3, 0, 8), (4, 0, 8), (5, 0, 4), (5, 4, 8)]
NP = len(CP)
ORDER = [
    "g0 f3 f0 f4", "f1 g4 c3 g1", "f2 F3 F0 F4", "G4 F2 G0 C5", "D0 F1 f5 R0", "I0 C1 g3 c2",
    "G1 D4 g2 D1", "F5 C0 c1 R4", "c5 I1 Q0 f6", "C6 R1 D3 D2", "c6 A1 G2 c0", "g5 C3 A2 G3",
    "f7 R2 A3 c4", "C2 A4 R3 V0", "D5 A5 C4 F6", "a V1 T0 G5", "V2 g6 Q1 g7", "T1 V3 T2 S0",
    "R5 B1 B2 V4", "V5 T3 V6 X0", "T4 B3 X1 F7", "D6 G6 T5 T6", "Y0 G7 R6 X2", "B4 D7 X3 R7",
    "B5 X4 Y2 o", "X5 Y4 Y1 Y3", "Y5",
]
MODES = [0, 2, 0, 2, 2, 2, 3, 3]
W, T2, JW, HW = 128, 256, 384, 768


def dot(a, b):
    return jnp.dot(a, b, precision=lax.Precision.HIGHEST, preferred_element_type=F32)


def kernel(l_hbm, out, lt, c0, xa, xb, bx, tt, db, oa, xc, oc, zz, acc, accx, ys,
           loc, snd, rcv, csnd, crcv, tsnd, trcv, osnd, orcv, bsnd, brcv, bloc, misc_s, misc_r, osem):
    row = lax.axis_index("row")
    y = lax.axis_index("col")
    x = row // 2
    k = row % 2
    ox, ok, oy = 1 - x, 1 - k, 1 - y
    sid = {"row": 2 * x + ok, "col": y}
    xid = {"row": 2 * ox + k, "col": y}
    yid = {"row": row, "col": oy}

    def way(c, core):
        return (core, 1 - core, 1, 0)[MODES[c]]

    def first(c):
        v = way(c, k)
        return {"row": row + (1 - v) * 2 * (1 - 2 * x), "col": y + v * (1 - 2 * y)}

    def second(c):
        v = 1 - way(c, k)
        return {"row": row + (1 - v) * 2 * (1 - 2 * x), "col": y + v * (1 - 2 * y)}

    def from_first(c, core):
        v = way(c, core)
        return y + v * (1 - 2 * y), x + (1 - v) * (1 - 2 * x)

    def from_second(c, core):
        v = 1 - way(c, core)
        return y + v * (1 - 2 * y), x + (1 - v) * (1 - 2 * x)

    started = []

    def remote(src, dst, ss, rs, dev):
        cp = pltpu.make_async_remote_copy(src_ref=src, dst_ref=dst, send_sem=ss, recv_sem=rs,
                                          device_id=dev, device_id_type=MESH)
        return cp

    def piece(c, q, p, xs):
        a, b = CHUNKS[c]
        return lt.at[a:b, q, p, :, xs, :, :]

    def put(c, kind, q, xs, dev):
        ref = piece(c, q, k, xs)
        cp = remote(ref, ref, snd.at[c, kind], rcv.at[c, kind], dev)
        cp.start()
        started.append(cp)

    def got(c, kind, q, p, xs):
        ref = piece(c, q, p, xs)
        remote(ref, ref, snd.at[c, kind], rcv.at[c, kind], sid).wait_recv()

    def local_copies(c):
        a, b = CHUNKS[c]
        return [pltpu.make_async_copy(l_hbm.at[8 * i:8 * i + 8, :, W * j:W * j + W],
                                      lt.at[a + n, y, k, :, x, :, :], loc.at[a + n])
                for n, (i, j) in enumerate(TILES[a:b])]

    barrier = pltpu.get_barrier_semaphore()
    for dev in (xid, yid, sid):
        pl.semaphore_signal(barrier, inc=1, device_id=dev, device_id_type=MESH)
    steps = [(name[0], int(name[1:] or 0)) for group in ORDER for name in group.split()]
    c0load = pltpu.make_async_copy(l_hbm.at[48:96, :, 0:HW], c0.at[y, k], loc.at[42])
    loads = {}
    for what, n in steps:
        if what in "fg" and n not in loads:
            loads[n] = local_copies(n)
            for cp in loads[n]:
                cp.start()
        if what in "cC" and 42 not in loads:
            c0load.start()
            loads[42] = [c0load]
    pl.semaphore_wait(barrier, 3)

    def loaded(c):
        for cp in loads.pop(c, []):
            cp.wait()

    def own_first(c):
        loaded(c)
        put(c, NF, y, x, first(c))
        put(c, SO, y, x, sid)

    def own_second(c):
        loaded(c)
        put(c, NG, y, x, second(c))

    def cref(n, q, p):
        s, m0, m1 = CP[n]
        return c0.at[q, p, 8 * s + m0:8 * s + m1]

    def cput(n, kind, q, dev):
        ref = cref(n, q, k)
        return remote(ref, ref, csnd.at[n, kind], crcv.at[n, kind], dev)

    def cgot(n, kind, q, p):
        ref = cref(n, q, p)
        remote(ref, ref, csnd.at[n, kind], crcv.at[n, kind], sid).wait_recv()

    def clear():
        xa[...] = jnp.zeros(xa.shape, F32)
        xb[...] = jnp.zeros(xb.shape, F32)
        zz[...] = jnp.zeros(zz.shape, F32)

    def serve_f(c):
        q, xs = from_first(c, k)
        got(c, NF, q, k, xs)
        put(c, ND, q, xs, second(c))
        put(c, SF, q, xs, sid)

    def serve_g(c):
        q, xs = from_second(c, k)
        got(c, NG, q, k, xs)
        put(c, SG, q, xs, sid)

    def serve_d(c):
        got(c, ND, oy, k, ox)
        put(c, SD, oy, ox, sid)

    def ready(c):
        got(c, SO, y, ok, x)
        q, xs = from_first(c, ok)
        got(c, SF, q, ok, xs)
        q, xs = from_second(c, ok)
        got(c, SG, q, ok, xs)
        got(c, SD, oy, ok, ox)

    lane = lax.broadcasted_iota(jnp.int32, (8, W), 1)
    grp = lane // 16
    G6 = 3
    lane48 = lax.broadcasted_iota(jnp.int32, (8 * G6, W), 1)
    sub48 = lax.broadcasted_iota(jnp.int32, (8 * G6, W), 0) % 8
    base48 = (lane48 // 16) * 16
    def rowcast(v, e):
        v3 = v.reshape(G6, 8, W)[:, e:e + 1, :]
        return jnp.broadcast_to(v3, (G6, 8, W)).reshape(8 * G6, W)

    def dtile(half, g):
        return TIDX[6 * half, 6 * half] + 2 * g + k

    def substitute(half):
        sub = {}
        for p in range(2):
            for sg in range(2):
                for q in range(2):
                    rows = []
                    for g in range(G6):
                        v = jnp.zeros((8, W), F32)
                        for m in range(8):
                            v = jnp.where(grp == m, lt[dtile(half, g), q, p, m, sg], v)
                        rows.append(v)
                    sub[2 * sg + p, q] = jnp.concatenate(rows, axis=0)
        yv = {}
        for be in range(4):
            for q in range(2):
                if be % 2 == q:
                    yv[be, q] = jnp.where(lane48 % 16 == 8 * (be // 2) + sub48, 1.0, 0.0).astype(F32)
                else:
                    yv[be, q] = jnp.zeros((8 * G6, W), F32)

        for be in range(4):
            for e in range(8):
                idx = base48 + (8 * (be // 2) + e)
                gs = {b2: jnp.take_along_axis(sub[b2, be % 2], idx, axis=1, mode="promise_in_bounds")
                      for b2 in range(be, 4)}
                rinv = 1.0 / rowcast(gs[be], e)
                for q in range(2):
                    piv = rowcast(yv[be, q], e) * rinv
                    for b2 in range(be, 4):
                        new = yv[b2, q] - gs[b2] * piv
                        if b2 == be:
                            new = jnp.where(sub48 > e, new, jnp.where(sub48 == e, piv, yv[b2, q]))
                        yv[b2, q] = new
        for be in range(4):
            for q in range(2):
                ys[be, q] = yv[be, q].reshape(G6, 8, W)

    lane256 = lax.broadcasted_iota(jnp.int32, (8, T2), 1) % W

    def invert(half, count=G6):
        dd, ll = [], []
        for n in range(count):
            g = n
            rows = []
            for p in range(2):
                for m in range(8):
                    for sg in range(2):
                        parts = [jnp.where(grp == m, ys[2 * sg + p, q, g], 0.0) for q in range(2)]
                        rows.append(jnp.concatenate(parts, axis=1))
            dd.append(rows)
            ll.append([jnp.concatenate([lt[dtile(half, g), q, p, m, sg] for q in range(2)], axis=1)
                       for p in range(2) for m in range(8) for sg in range(2)])
        for h8 in (2, 4, 8):
            odd = [b for b in range(32) if (b % 16) // h8 % 2 == 1]
            zero = jnp.zeros((8, T2), F32)
            tds = []
            for n in range(count):
                mo = [jnp.where(lane256 // (8 * h8) == (b % 16) // h8 - 1, ll[n][b], 0.0) for b in odd]
                tds.append(dot(jnp.concatenate(mo, axis=0), jnp.concatenate(dd[n], axis=0)))
            for n in range(count):
                tfull = [zero] * 32
                for o, b in enumerate(odd):
                    tfull[b] = tds[n][8 * o:8 * o + 8]
                xo = dot(jnp.concatenate([dd[n][b] for b in odd], axis=0), jnp.concatenate(tfull, axis=0))
                for o, b in enumerate(odd):
                    dd[n][b] = dd[n][b] - xo[8 * o:8 * o + 8]
        for n in range(count):
            db[G6 * half + n, k] = jnp.concatenate(dd[n], axis=0)
        dbcopy(half, k).start()

    def dbcopy(half, kk):
        ref = db.at[G6 * half:G6 * half + G6, kk]
        return remote(ref, ref, misc_s.at[half], misc_r.at[half], sid)

    def ltile(t):
        return jnp.concatenate([lt[t, q].reshape(T2, W) for q in range(2)], axis=1)

    need = [0, 1, 1, 0, 0, 1]

    def place_a(i):
        @pl.when(k == need[i])
        def _():
            t = i // 2
            d = db[i // 2, i % 2, :, pl.ds(pl.multiple_of(y * W, W), W)]
            xa[i, :, :, :, :, W * t:W * t + W] = d.reshape(2, 8, 2, 8, W)

    def step_a(i):
        for j in range(i):
            n = W * (j // 2 + 1)
            d = dot(ltile(TIDX[i, j]), xa[j, :, :, :, :, 0:n].reshape(T2, n))
            n0 = 0 if j == 0 else W * ((j - 1) // 2 + 1)
            if n0:
                acc[:, 0:n0] = acc[:, 0:n0] + d[:, 0:n0]
            if n > n0:
                acc[:, n0:n] = d[:, n0:n]
        n = W * ((i + 1) // 2)
        r = -dot(db[i // 2, i % 2], acc[:, 0:n])
        xa[i, :, :, :, :, 0:n] = r.reshape(2, 8, 2, 8, n)
        place_a(i)

    def place_b(i):
        d = db[3 + i // 2, i % 2, :, pl.ds(pl.multiple_of(k * W, W), W)]
        xb[i, :, :, :, :, W * i:W * i + W] = d.reshape(2, 8, 2, 8, W)

    def step_b(i):
        for j in range(i):
            n = W * (j + 1)
            d = dot(ltile(TIDX[i + 6, j + 6]), xb[j, :, :, :, :, 0:n].reshape(T2, n))
            if j:
                acc[:, 0:n - W] = acc[:, 0:n - W] + d[:, 0:n - W]
            acc[:, n - W:n] = d[:, n - W:n]
        n = W * i
        r = -dot(db[3 + i // 2, i % 2], acc[:, 0:n])
        xb[i, :, :, :, :, 0:n] = r.reshape(2, 8, 2, 8, n)
        place_b(i)

    outs = []

    def put_out(src, dst):
        cp = pltpu.make_async_copy(src, dst, osem.at[len(outs)])
        cp.start()
        outs.append(cp)

    def jcol(t, kk):
        return [kk, 3 - kk, 4 + kk][t]

    def lanes(t, kk):
        return pl.ds(pl.multiple_of(W * jcol(t, kk), W), W)

    oacopy = remote(xa.at[:, ok, :, x, :, :], oa, misc_s.at[2], misc_r.at[2], sid)

    def finish_a():
        oacopy.start()
        for i in range(6):
            put_out(zz, out.at[i, :, :, HW:2 * HW])
        for t in range(3):
            put_out(xa.at[:, k, :, x, :, W * t:W * t + W], out.at[0:6, :, :, lanes(t, k)])

    def finish_oa():
        remote(oa, oa, misc_s.at[2], misc_r.at[2], sid).wait_recv()
        for t in range(3):
            put_out(oa.at[:, :, :, W * t:W * t + W], out.at[0:6, :, :, lanes(t, ok)])

    def bxcopy(i, kk):
        return remote(xb.at[i, :, :, x, :, :], bx.at[kk, i], bsnd.at[i], brcv.at[i], sid)

    def bxlocal(i):
        return pltpu.make_async_copy(xb.at[i, :, :, x, :, :], bx.at[k, i], bloc.at[i])

    def send_b(i):
        bxcopy(i, k).start()
        bxlocal(i).start()

    def get_b(i):
        bxlocal(i).wait()
        bxcopy(i, ok).wait_recv()
        put_out(bx.at[y, i, k], out.at[6 + i, :, :, HW:2 * HW])

    def tcopy(n, xs):
        s, m0, m1 = CP[n]
        ref = tt.at[s, :, m0:m1, xs, :, :]
        return remote(ref, ref, tsnd.at[n], trcv.at[n], xid)

    def serve_c(n):
        cgot(n, 0, oy, k)
        cput(n, 2, oy, sid).start()

    def do_t(n):
        s, m0, m1 = CP[n]
        g = 8 * (m1 - m0)
        cgot(n, 1, y, ok)
        cgot(n, 2, oy, ok)
        for u in range(3):
            w = W * (u + 1)
            parts = []
            for j in (2 * u, 2 * u + 1):
                for q in range(2):
                    parts.append(c0[q, :, 8 * s + m0:8 * s + m1, :, W * j:W * j + W].reshape(2 * g, W))
            rhs = jnp.concatenate([xa[2 * u + e, :, :, :, :, 0:w].reshape(T2, w) for e in range(2)], axis=0)
            d = dot(jnp.concatenate(parts, axis=1), rhs)
            if u:
                acc[0:2 * g, 0:w - W] = acc[0:2 * g, 0:w - W] + d[:, 0:w - W]
            acc[0:2 * g, w - W:w] = d[:, w - W:w]
        tt[s, :, m0:m1, x, :, :] = acc[0:2 * g, 0:JW].reshape(2, m1 - m0, 8, JW)
        tcopy(n, x).start()

    def xpart(s, u):
        ln = pl.ds(pl.multiple_of(u * W, W), W)
        lhs = jnp.concatenate([bx[q, s, :, :, :, ln].reshape(W, W) for q in range(2)], axis=1)
        return dot(lhs, tt[u].reshape(T2, JW))

    def do_x(s):
        get_b(s)
        accx[...] = jnp.zeros((W, JW), F32)

        def body(u, carry):
            accx[...] = accx[...] - xpart(s, u)
            return carry

        lax.fori_loop(0, s, body, 0)
        for n in range(NP):
            if CP[n][0] == s:
                tcopy(n, ox).wait_recv()
        xc[s] = (accx[...] - xpart(s, s)).reshape(2, 8, 8, JW)
        remote(xc.at[s, ok], oc.at[s], osnd.at[s], orcv.at[s], sid).start()
        for t in range(3):
            put_out(xc.at[s, k, :, :, W * t:W * t + W], out.at[6 + s, :, :, lanes(t, k)])

    def finish_x(s):
        remote(oc.at[s], oc.at[s], osnd.at[s], orcv.at[s], sid).wait_recv()
        for t in range(3):
            put_out(oc.at[s, :, :, W * t:W * t + W], out.at[6 + s, :, :, lanes(t, ok)])

    def inv(half):
        substitute(half)
        invert(half)

    def get_d(half):
        dbcopy(half, ok).wait_recv()
        (place_b if half else place_a)(0)

    def do_b(i):
        step_b(i)
        send_b(i)

    def csend(n):
        loaded(42)
        cput(n, 0, y, yid).start()

    def csib(n):
        loaded(42)
        cput(n, 1, y, sid).start()

    run = {"f": own_first, "g": own_second, "F": serve_f, "G": serve_g, "D": serve_d, "R": ready, "I": inv,
           "Q": get_d, "A": step_a, "B": do_b, "S": send_b, "C": csend, "c": csib, "V": serve_c, "T": do_t,
           "X": do_x, "Y": finish_x, "a": lambda _: finish_a(), "o": lambda _: finish_oa()}
    cleared = False
    for what, n in steps:
        if what in "FGDR" and not cleared:
            clear()
            cleared = True
        with jax.named_scope(f"{what}{n}"):
            run[what](n)

    for cp in started:
        cp.wait_send()
    for n in range(NP):
        cput(n, 0, y, yid).wait_send()
        cput(n, 1, y, sid).wait_send()
        cput(n, 2, oy, sid).wait_send()
        tcopy(n, x).wait_send()
    for s in range(6):
        bxcopy(s, k).wait_send()
        remote(xc.at[s, ok], oc.at[s], osnd.at[s], orcv.at[s], sid).wait_send()
    dbcopy(0, k).wait_send()
    dbcopy(1, k).wait_send()
    oacopy.wait_send()
    for cp in outs:
        cp.wait()


def solution(mesh):
    spec = P(("batch", "row"), "col")
    vm = lambda *shape: pltpu.VMEM(shape, F32)
    dma = lambda *shape: pltpu.SemaphoreType.DMA(shape)

    def body(local_l):
        got = pl.pallas_call(
            kernel,
            name="tri_inverse",
            out_shape=jax.ShapeDtypeStruct((12, 8, 8, 1536), F32),
            in_specs=[pl.BlockSpec(memory_space=pl.ANY)],
            out_specs=pl.BlockSpec(memory_space=pl.ANY),
            scratch_shapes=[
                vm(42, 2, 2, 8, 2, 8, W),
                vm(2, 2, 48, 8, HW),
                vm(6, 2, 8, 2, 8, JW),
                vm(6, 2, 8, 2, 8, HW),
                vm(2, 6, 2, 8, 8, HW),
                vm(6, 2, 8, 2, 8, JW),
                vm(6, 2, T2, T2),
                vm(6, 8, 8, JW),
                vm(6, 2, 8, 8, JW),
                vm(6, 8, 8, JW),
                vm(8, 8, HW),
                vm(T2, HW),
                vm(W, JW),
                vm(4, 2, 3, 8, W),
                dma(43), dma(NC, 7), dma(NC, 7), dma(NP, 3), dma(NP, 3), dma(NP), dma(NP),
                dma(6), dma(6), dma(6), dma(6), dma(6), dma(3), dma(3), dma(64),
            ],
            compiler_params=pltpu.CompilerParams(
                collective_id=0, has_side_effects=True, vmem_limit_bytes=47 * 2**20),
        )(local_l.reshape(96, 8, 1536))
        return got.reshape(HW, 1536)

    return jax.shard_map(body, mesh=mesh, in_specs=(spec,), out_specs=spec, check_vma=False)
```

```python
import functools

import jax
import jax.numpy as jnp
from jax import lax
from jax.experimental import pallas as pl
from jax.experimental.pallas import tpu as pltpu
from jax.sharding import PartitionSpec as P

MESH = pl.DeviceIdType.MESH
F32 = jnp.float32

DIAG = [(i, i) for i in range(12)]
OFF_A = [(i, j) for i in range(1, 6) for j in range(i)]
OFF_B = [(i + 6, j + 6) for i in range(1, 6) for j in range(i)]
TILES = DIAG[:6] + OFF_A + DIAG[6:] + OFF_B
TIDX = {ij: t for t, ij in enumerate(TILES)}
CHUNKS = [(0, 6), (6, 12), (12, 16), (16, 21), (21, 27), (27, 33), (33, 37), (37, 42)]
NC = len(CHUNKS)
NF, NG, ND, SO, SF, SG, SD = range(7)
CP = [(0, 0, 8), (1, 0, 8), (2, 0, 8), (3, 0, 8), (4, 0, 8), (5, 0, 4), (5, 4, 8)]
NP = len(CP)
TG = [(0, 1), (2, 3), (4,), (5,), (6,)]
ORDER = [
    "g0 f3 f0 f4", "f1 g4 c3 g1", "f2 F3 F0 F4", "G4 F2 G0 C5", "D0 F1 f5 R0", "I0 C1 g3 c2",
    "G1 D4 g2 D1", "F5 C0 c1 R4", "c5 I1 Q0 f6", "C6 R1 D3 D2", "c6 A1 G2 c0", "g5 C3 A2 G3",
    "f7 R2 A3 c4", "C2 A4 R3 V0", "D5 A5 C4 F6", "a V1 G5 V2", "g6 Q1 g7 T0", "V3 S0 R5 B1",
    "B2 V4 V5 T1", "V6 T2 B3 P0", "X0 X1 F7 D6", "G6 T3 T4 G7", "R6 B4 D7 P1", "X2 X3 R7 B5",
    "o P2 X4 X5", "Y0 Y1 Y2 Y3", "Y4 Y5",
]
MODES = [0, 2, 0, 2, 2, 2, 3, 3]
W, T2, JW, HW = 128, 256, 384, 768


def dot(a, b):
    return jnp.dot(a, b, precision=lax.Precision.HIGHEST, preferred_element_type=F32)


def kernel(l_hbm, out, lt, c0, xa, xb, bx, tt, db, oa, xc, oc, zz, acc, accx, ys,
           loc, snd, rcv, crcv, trcv, orcv, brcv, bloc, misc_r, osem):
    row = lax.axis_index("row")
    y = lax.axis_index("col")
    x = row // 2
    k = row % 2
    ox, ok, oy = 1 - x, 1 - k, 1 - y
    sid = {"row": 2 * x + ok, "col": y}
    xid = {"row": 2 * ox + k, "col": y}
    yid = {"row": row, "col": oy}

    def way(c, core):
        return (core, 1 - core, 1, 0)[MODES[c]]

    def first(c):
        v = way(c, k)
        return {"row": row + (1 - v) * 2 * (1 - 2 * x), "col": y + v * (1 - 2 * y)}

    def second(c):
        v = 1 - way(c, k)
        return {"row": row + (1 - v) * 2 * (1 - 2 * x), "col": y + v * (1 - 2 * y)}

    def from_first(c, core):
        v = way(c, core)
        return y + v * (1 - 2 * y), x + (1 - v) * (1 - 2 * x)

    def from_second(c, core):
        v = 1 - way(c, core)
        return y + v * (1 - 2 * y), x + (1 - v) * (1 - 2 * x)

    started = []

    def remote(src, dst, ss, rs, dev):
        cp = pltpu.make_async_remote_copy(src_ref=src, dst_ref=dst, send_sem=ss, recv_sem=rs,
                                          device_id=dev, device_id_type=MESH)
        return cp

    def piece(c, q, p, xs):
        a, b = CHUNKS[c]
        return lt.at[a:b, q, p, :, xs, :, :]

    def put(c, kind, q, xs, dev):
        ref = piece(c, q, k, xs)
        cp = remote(ref, ref, snd.at[0], rcv.at[c, kind], dev)
        cp.start()
        started.append(cp)

    def got(c, kind, q, p, xs):
        ref = piece(c, q, p, xs)
        remote(ref, ref, snd.at[0], rcv.at[c, kind], sid).wait_recv()

    def local_copies(c):
        a, b = CHUNKS[c]
        return [pltpu.make_async_copy(l_hbm.at[8 * i:8 * i + 8, :, W * j:W * j + W],
                                      lt.at[a + n, y, k, :, x, :, :], loc.at[c])
                for n, (i, j) in enumerate(TILES[a:b])]

    barrier = pltpu.get_barrier_semaphore()
    for dev in (xid, yid, sid):
        pl.semaphore_signal(barrier, inc=1, device_id=dev, device_id_type=MESH)
    steps = [(name[0], int(name[1:] or 0)) for group in ORDER for name in group.split()]
    c0load = pltpu.make_async_copy(l_hbm.at[48:96, :, 0:HW], c0.at[y, k], loc.at[NC])
    loads = {}
    for what, n in steps:
        if what in "fg" and n not in loads:
            loads[n] = local_copies(n)
            for cp in loads[n]:
                cp.start()
        if what in "cC" and 42 not in loads:
            c0load.start()
            loads[42] = [c0load]
    pl.semaphore_wait(barrier, 3)

    def loaded(c):
        for cp in loads.pop(c, []):
            cp.wait()

    def own_first(c):
        loaded(c)
        put(c, NF, y, x, first(c))
        put(c, SO, y, x, sid)

    def own_second(c):
        loaded(c)
        put(c, NG, y, x, second(c))

    def cref(n, q, p):
        s, m0, m1 = CP[n]
        return c0.at[q, p, 8 * s + m0:8 * s + m1]

    def cput(n, kind, q, dev):
        ref = cref(n, q, k)
        return remote(ref, ref, snd.at[0], crcv.at[n, kind], dev)

    def cgot(n, kind, q, p):
        ref = cref(n, q, p)
        remote(ref, ref, snd.at[0], crcv.at[n, kind], sid).wait_recv()

    def clear():
        xa[...] = jnp.zeros(xa.shape, F32)
        xb[...] = jnp.zeros(xb.shape, F32)
        zz[...] = jnp.zeros(zz.shape, F32)

    def serve_f(c):
        q, xs = from_first(c, k)
        got(c, NF, q, k, xs)
        put(c, ND, q, xs, second(c))
        put(c, SF, q, xs, sid)

    def serve_g(c):
        q, xs = from_second(c, k)
        got(c, NG, q, k, xs)
        put(c, SG, q, xs, sid)

    def serve_d(c):
        got(c, ND, oy, k, ox)
        put(c, SD, oy, ox, sid)

    def ready(c):
        got(c, SO, y, ok, x)
        q, xs = from_first(c, ok)
        got(c, SF, q, ok, xs)
        q, xs = from_second(c, ok)
        got(c, SG, q, ok, xs)
        got(c, SD, oy, ok, ox)

    lane = lax.broadcasted_iota(jnp.int32, (8, W), 1)
    grp = lane // 16
    G6 = 3
    lane48 = lax.broadcasted_iota(jnp.int32, (8 * G6, W), 1)
    sub48 = lax.broadcasted_iota(jnp.int32, (8 * G6, W), 0) % 8
    base48 = (lane48 // 16) * 16
    def rowcast(v, e):
        v3 = v.reshape(G6, 8, W)[:, e:e + 1, :]
        return jnp.broadcast_to(v3, (G6, 8, W)).reshape(8 * G6, W)

    def dtile(half, g):
        return TIDX[6 * half, 6 * half] + 2 * g + k

    def substitute(half):
        sub = {}
        for p in range(2):
            for sg in range(2):
                for q in range(2):
                    rows = []
                    for g in range(G6):
                        v = jnp.zeros((8, W), F32)
                        for m in range(8):
                            v = jnp.where(grp == m, lt[dtile(half, g), q, p, m, sg], v)
                        rows.append(v)
                    sub[2 * sg + p, q] = jnp.concatenate(rows, axis=0)
        yv = {}
        for be in range(4):
            for q in range(2):
                if be % 2 == q:
                    yv[be, q] = jnp.where(lane48 % 16 == 8 * (be // 2) + sub48, 1.0, 0.0).astype(F32)
                else:
                    yv[be, q] = jnp.zeros((8 * G6, W), F32)

        for be in range(4):
            for e in range(8):
                idx = base48 + (8 * (be // 2) + e)
                gs = {b2: jnp.take_along_axis(sub[b2, be % 2], idx, axis=1, mode="promise_in_bounds")
                      for b2 in range(be, 4)}
                rinv = 1.0 / rowcast(gs[be], e)
                for q in range(2):
                    piv = rowcast(yv[be, q], e) * rinv
                    for b2 in range(be, 4):
                        new = yv[b2, q] - gs[b2] * piv
                        if b2 == be:
                            new = jnp.where(sub48 > e, new, jnp.where(sub48 == e, piv, yv[b2, q]))
                        yv[b2, q] = new
        for be in range(4):
            for q in range(2):
                ys[be, q] = yv[be, q].reshape(G6, 8, W)

    lane256 = lax.broadcasted_iota(jnp.int32, (8, T2), 1) % W

    def invert(half, count=G6):
        dd, ll = [], []
        for n in range(count):
            g = n
            rows = []
            for p in range(2):
                for m in range(8):
                    for sg in range(2):
                        parts = [jnp.where(grp == m, ys[2 * sg + p, q, g], 0.0) for q in range(2)]
                        rows.append(jnp.concatenate(parts, axis=1))
            dd.append(rows)
            ll.append([jnp.concatenate([lt[dtile(half, g), q, p, m, sg] for q in range(2)], axis=1)
                       for p in range(2) for m in range(8) for sg in range(2)])
        for h8 in (2, 4, 8):
            odd = [b for b in range(32) if (b % 16) // h8 % 2 == 1]
            zero = jnp.zeros((8, T2), F32)
            tds = []
            for n in range(count):
                mo = [jnp.where(lane256 // (8 * h8) == (b % 16) // h8 - 1, ll[n][b], 0.0) for b in odd]
                tds.append(dot(jnp.concatenate(mo, axis=0), jnp.concatenate(dd[n], axis=0)))
            for n in range(count):
                tfull = [zero] * 32
                for o, b in enumerate(odd):
                    tfull[b] = tds[n][8 * o:8 * o + 8]
                xo = dot(jnp.concatenate([dd[n][b] for b in odd], axis=0), jnp.concatenate(tfull, axis=0))
                for o, b in enumerate(odd):
                    dd[n][b] = dd[n][b] - xo[8 * o:8 * o + 8]
        for n in range(count):
            db[G6 * half + n, k] = jnp.concatenate(dd[n], axis=0)
        dbcopy(half, k).start()

    def dbcopy(half, kk):
        ref = db.at[G6 * half:G6 * half + G6, kk]
        return remote(ref, ref, snd.at[0], misc_r.at[half], sid)

    def ltile(t):
        return jnp.concatenate([lt[t, q].reshape(T2, W) for q in range(2)], axis=1)

    need = [0, 1, 1, 0, 0, 1]

    def place_a(i):
        @pl.when(k == need[i])
        def _():
            t = i // 2
            d = db[i // 2, i % 2, :, pl.ds(pl.multiple_of(y * W, W), W)]
            xa[i, :, :, :, :, W * t:W * t + W] = d.reshape(2, 8, 2, 8, W)

    def step_a(i):
        for j in range(i):
            n = W * (j // 2 + 1)
            d = dot(ltile(TIDX[i, j]), xa[j, :, :, :, :, 0:n].reshape(T2, n))
            n0 = 0 if j == 0 else W * ((j - 1) // 2 + 1)
            if n0:
                acc[:, 0:n0] = acc[:, 0:n0] + d[:, 0:n0]
            if n > n0:
                acc[:, n0:n] = d[:, n0:n]
        n = W * ((i + 1) // 2)
        r = -dot(db[i // 2, i % 2], acc[:, 0:n])
        xa[i, :, :, :, :, 0:n] = r.reshape(2, 8, 2, 8, n)
        place_a(i)

    def place_b(i):
        d = db[3 + i // 2, i % 2, :, pl.ds(pl.multiple_of(k * W, W), W)]
        xb[i, :, :, :, :, W * i:W * i + W] = d.reshape(2, 8, 2, 8, W)

    def step_b(i):
        for j in range(i):
            n = W * (j + 1)
            d = dot(ltile(TIDX[i + 6, j + 6]), xb[j, :, :, :, :, 0:n].reshape(T2, n))
            if j:
                acc[:, 0:n - W] = acc[:, 0:n - W] + d[:, 0:n - W]
            acc[:, n - W:n] = d[:, n - W:n]
        n = W * i
        r = -dot(db[3 + i // 2, i % 2], acc[:, 0:n])
        xb[i, :, :, :, :, 0:n] = r.reshape(2, 8, 2, 8, n)
        place_b(i)

    outs = []

    def put_out(src, dst):
        cp = pltpu.make_async_copy(src, dst, osem.at[0])
        cp.start()
        outs.append(cp)

    def jcol(t, kk):
        return [kk, 3 - kk, 4 + kk][t]

    def lanes(t, kk):
        return pl.ds(pl.multiple_of(W * jcol(t, kk), W), W)

    oacopy = remote(xa.at[:, ok, :, x, :, :], oa, snd.at[0], misc_r.at[2], sid)

    def finish_a():
        oacopy.start()
        for i in range(6):
            put_out(zz, out.at[i, :, :, HW:2 * HW])
        for t in range(3):
            put_out(xa.at[:, k, :, x, :, W * t:W * t + W], out.at[0:6, :, :, lanes(t, k)])

    def finish_oa():
        remote(oa, oa, snd.at[0], misc_r.at[2], sid).wait_recv()
        for t in range(3):
            put_out(oa.at[:, :, :, W * t:W * t + W], out.at[0:6, :, :, lanes(t, ok)])

    def bxcopy(i, kk):
        return remote(xb.at[i, :, :, x, :, :], bx.at[kk, i], snd.at[0], brcv.at[i], sid)

    def bxlocal(i):
        return pltpu.make_async_copy(xb.at[i, :, :, x, :, :], bx.at[k, i], bloc.at[i])

    def send_b(i):
        bxcopy(i, k).start()
        bxlocal(i).start()

    def get_b(i):
        bxlocal(i).wait()
        bxcopy(i, ok).wait_recv()
        put_out(bx.at[y, i, k], out.at[6 + i, :, :, HW:2 * HW])

    def tcopy(n, xs):
        s, m0, m1 = CP[n]
        ref = tt.at[s, :, m0:m1, xs, :, :]
        return remote(ref, ref, snd.at[0], trcv.at[n], xid)

    def serve_c(n):
        cgot(n, 0, oy, k)
        cput(n, 2, oy, sid).start()

    def do_t(h):
        group = TG[h]
        for n in group:
            cgot(n, 1, y, ok)
            cgot(n, 2, oy, ok)
        lo = 8 * CP[group[0]][0] + CP[group[0]][1]
        hi = 8 * CP[group[-1]][0] + CP[group[-1]][2]
        g = 8 * (hi - lo)
        for u in range(3):
            w = W * (u + 1)
            parts = []
            for j in (2 * u, 2 * u + 1):
                for q in range(2):
                    parts.append(c0[q, :, lo:hi, :, W * j:W * j + W].reshape(2 * g, W))
            rhs = jnp.concatenate([xa[2 * u + e, :, :, :, :, 0:w].reshape(T2, w) for e in range(2)], axis=0)
            d = dot(jnp.concatenate(parts, axis=1), rhs)
            if u:
                acc[0:2 * g, 0:w - W] = acc[0:2 * g, 0:w - W] + d[:, 0:w - W]
            acc[0:2 * g, w - W:w] = d[:, w - W:w]
        for n in group:
            s, m0, m1 = CP[n]
            at = 8 * (8 * s + m0 - lo)
            size = 8 * (m1 - m0)
            for p in range(2):
                r = acc[p * g + at:p * g + at + size, 0:JW]
                tt[s, p, m0:m1, x, :, :] = r.reshape(m1 - m0, 8, JW)
            tcopy(n, x).start()

    def tgot(s):
        for n in range(NP):
            if CP[n][0] == s:
                tcopy(n, ox).wait_recv()

    def bpart(s, count, u, nu):
        parts = []
        for e in range(nu):
            ln = pl.ds(pl.multiple_of((u + e) * W, W), W)
            for q in range(2):
                parts.append(bx[q, s:s + count, :, :, :, ln].reshape(count * W, W))
        rhs = jnp.concatenate([tt[u + e].reshape(T2, JW) for e in range(nu)], axis=0)
        return dot(jnp.concatenate(parts, axis=1), rhs)

    def do_p(a):
        for s in (2 * a, 2 * a + 1):
            get_b(s)

        def body(it, carry):
            accx[...] = accx[...] - bpart(2 * a, 2, 2 * it, 2)
            return carry

        if a > 1:
            accx[...] = jnp.zeros((T2, JW), F32)
            lax.fori_loop(0, a, body, 0)
        elif a == 1:
            accx[...] = -bpart(2, 2, 0, 2)

    def do_x(s):
        tgot(s)
        if s == 0:
            accx[...] = -bpart(0, 2, 0, 1)
        elif s % 2 == 0:
            accx[...] = accx[...] - bpart(s, 2, s, 1)
        else:
            accx[W:, :] = accx[W:, :] - bpart(s, 1, s, 1)
        at = W * (s % 2)
        xc[s] = accx[at:at + W, :].reshape(2, 8, 8, JW)
        remote(xc.at[s, ok], oc.at[s], snd.at[0], orcv.at[s], sid).start()
        for t in range(3):
            put_out(xc.at[s, k, :, :, W * t:W * t + W], out.at[6 + s, :, :, lanes(t, k)])

    def finish_x(s):
        remote(oc.at[s], oc.at[s], snd.at[0], orcv.at[s], sid).wait_recv()
        for t in range(3):
            put_out(oc.at[s, :, :, W * t:W * t + W], out.at[6 + s, :, :, lanes(t, ok)])

    def inv(half):
        substitute(half)
        invert(half)

    def get_d(half):
        dbcopy(half, ok).wait_recv()
        (place_b if half else place_a)(0)

    def do_b(i):
        step_b(i)
        send_b(i)

    def csend(n):
        loaded(42)
        cput(n, 0, y, yid).start()

    def csib(n):
        loaded(42)
        cput(n, 1, y, sid).start()

    run = {"f": own_first, "g": own_second, "F": serve_f, "G": serve_g, "D": serve_d, "R": ready, "I": inv,
           "Q": get_d, "A": step_a, "B": do_b, "S": send_b, "C": csend, "c": csib, "V": serve_c, "T": do_t,
           "X": do_x, "P": do_p, "Y": finish_x, "a": lambda _: finish_a(), "o": lambda _: finish_oa()}
    cleared = False
    for what, n in steps:
        if what in "FGDR" and not cleared:
            clear()
            cleared = True
        with jax.named_scope(f"{what}{n}"):
            run[what](n)

    for cp in started:
        cp.wait_send()
    for n in range(NP):
        cput(n, 0, y, yid).wait_send()
        cput(n, 1, y, sid).wait_send()
        cput(n, 2, oy, sid).wait_send()
        tcopy(n, x).wait_send()
    for s in range(6):
        bxcopy(s, k).wait_send()
        remote(xc.at[s, ok], oc.at[s], snd.at[0], orcv.at[s], sid).wait_send()
    dbcopy(0, k).wait_send()
    dbcopy(1, k).wait_send()
    oacopy.wait_send()
    for cp in outs:
        cp.wait()


def solution(mesh):
    spec = P(("batch", "row"), "col")
    vm = lambda *shape: pltpu.VMEM(shape, F32)
    dma = lambda *shape: pltpu.SemaphoreType.DMA(shape)

    def body(local_l):
        got = pl.pallas_call(
            kernel,
            name="tri_inverse",
            out_shape=jax.ShapeDtypeStruct((12, 8, 8, 1536), F32),
            in_specs=[pl.BlockSpec(memory_space=pl.ANY)],
            out_specs=pl.BlockSpec(memory_space=pl.ANY),
            scratch_shapes=[
                vm(42, 2, 2, 8, 2, 8, W),
                vm(2, 2, 48, 8, HW),
                vm(6, 2, 8, 2, 8, JW),
                vm(6, 2, 8, 2, 8, HW),
                vm(2, 6, 2, 8, 8, HW),
                vm(6, 2, 8, 2, 8, JW),
                vm(6, 2, T2, T2),
                vm(6, 8, 8, JW),
                vm(6, 2, 8, 8, JW),
                vm(6, 8, 8, JW),
                vm(8, 8, HW),
                vm(T2, HW),
                vm(T2, JW),
                vm(4, 2, 3, 8, W),
                dma(NC + 1), dma(1), dma(NC, 7), dma(NP, 3), dma(NP), dma(6), dma(6), dma(6), dma(3), dma(1),
            ],
            compiler_params=pltpu.CompilerParams(
                collective_id=0, has_side_effects=True, vmem_limit_bytes=47 * 2**20),
        )(local_l.reshape(96, 8, 1536))
        return got.reshape(HW, 1536)

    return jax.shard_map(body, mesh=mesh, in_specs=(spec,), out_specs=spec, check_vma=False)
```

```python
import functools

import jax
import jax.numpy as jnp
from jax import lax
from jax.experimental import pallas as pl
from jax.experimental.pallas import tpu as pltpu
from jax.sharding import PartitionSpec as P

MESH = pl.DeviceIdType.MESH
F32 = jnp.float32

OFF_A = [(i, j) for i in range(1, 6) for j in range(i)]
OFF_B = [(i + 6, j + 6) for i in range(1, 6) for j in range(i)]
TILES = OFF_A + OFF_B
TIDX = {ij: t for t, ij in enumerate(TILES)}
CHUNKS = [None, (0, 6), (6, 10), (10, 15), None, (15, 21), (21, 25), (25, 30)]
NC = len(CHUNKS)
NF, NG, ND, SO, SF, SG, SD = range(7)
CP = [(0, 0, 8), (1, 0, 8), (2, 0, 8), (3, 0, 8), (4, 0, 8), (5, 0, 4), (5, 4, 8)]
NP = len(CP)
TG = [(0, 1), (2, 3), (4,), (5,), (6,)]
ORDER = [
    "f0 c5 g4 f3", "f4 g0 F3 f2", "f1 g2 G0 c4", "g1 F0 F4 F2", "f5 D0 f6 G1", "R0 D3 c0 c2",
    "G2 F1 I0 g3", "C0 C1 c1 Q0", "D4 g5 g6 G4", "C2 D2 R4 R2", "D1 F5 F6 G3", "c6 C3 R1 I1",
    "R3 A1 A2 V0", "A3 A4 V1 Q1", "G6 f7 A5 C4", "S0 G5 C5 T0", "c3 D5 V2 R5", "V3 B1 B2 C6",
    "T1 V4 F7 B3", "D6 g7 P0 V5", "T2 X0 T3 V6", "X1 P1 Y0 R6", "B4 Y1 D7 T4", "G7 R7 B5 X2",
    "X3 a0 P2 X4", "X5 o0 Y2 Y3", "Y4 Y5",
]
MODES = [0, 0, 2, 1, 2, 2, 2, 3]
W, T2, JW, HW = 128, 256, 384, 768


def dot(a, b):
    return jnp.dot(a, b, precision=lax.Precision.HIGHEST, preferred_element_type=F32)


def kernel(l_hbm, out, lt, ld, raw, c0, xa, xb, bx, tt, db, oa, xc, oc, zz, acc, accx, ys,
           loc, snd, rcv, crcv, trcv, orcv, brcv, bloc, misc_r, osem):
    row = lax.axis_index("row")
    y = lax.axis_index("col")
    x = row // 2
    k = row % 2
    ox, ok, oy = 1 - x, 1 - k, 1 - y
    sid = {"row": 2 * x + ok, "col": y}
    xid = {"row": 2 * ox + k, "col": y}
    yid = {"row": row, "col": oy}

    def way(c, core):
        return (core, 1 - core, 1, 0)[MODES[c]]

    def first(c):
        v = way(c, k)
        return {"row": row + (1 - v) * 2 * (1 - 2 * x), "col": y + v * (1 - 2 * y)}

    def second(c):
        v = 1 - way(c, k)
        return {"row": row + (1 - v) * 2 * (1 - 2 * x), "col": y + v * (1 - 2 * y)}

    def from_first(c, core):
        v = way(c, core)
        return y + v * (1 - 2 * y), x + (1 - v) * (1 - 2 * x)

    def from_second(c, core):
        v = 1 - way(c, core)
        return y + v * (1 - 2 * y), x + (1 - v) * (1 - 2 * x)

    started = []

    def remote(src, dst, ss, rs, dev):
        cp = pltpu.make_async_remote_copy(src_ref=src, dst_ref=dst, send_sem=ss, recv_sem=rs,
                                          device_id=dev, device_id_type=MESH)
        return cp

    def piece(c, q, p, xs):
        if CHUNKS[c] is None:
            return ld.at[c // 4, q, p, :, :, xs, :, :]
        a, b = CHUNKS[c]
        return lt.at[a:b, q, p, :, xs, :, :]

    def put(c, kind, q, xs, dev):
        ref = piece(c, q, k, xs)
        cp = remote(ref, ref, snd.at[0], rcv.at[c, kind], dev)
        cp.start()
        started.append(cp)

    def got(c, kind, q, p, xs):
        ref = piece(c, q, p, xs)
        remote(ref, ref, snd.at[0], rcv.at[c, kind], sid).wait_recv()

    def local_copies(c):
        if CHUNKS[c] is None:
            h = c // 4
            low, high = [], []
            for n in range(6):
                i = 6 * h + n
                cols = slice(W * i, W * i + W)
                low.append(pltpu.make_async_copy(l_hbm.at[8 * i:8 * i + 4, :, cols], raw.at[h, n], loc.at[c]))
                high.append(pltpu.make_async_copy(l_hbm.at[8 * i + 4:8 * i + 8, :, cols],
                                                  ld.at[h, y, k, n, :, x, :, :], loc.at[c]))
            return low + high
        a, b = CHUNKS[c]
        return [pltpu.make_async_copy(l_hbm.at[8 * i:8 * i + 8, :, W * j:W * j + W],
                                      lt.at[a + n, y, k, :, x, :, :], loc.at[c])
                for n, (i, j) in enumerate(TILES[a:b])]

    barrier = pltpu.get_barrier_semaphore()
    for dev in (xid, yid, sid):
        pl.semaphore_signal(barrier, inc=1, device_id=dev, device_id_type=MESH)
    steps = [(name[0], int(name[1:] or 0)) for group in ORDER for name in group.split()]
    c0load = pltpu.make_async_copy(l_hbm.at[48:96, :, 0:HW], c0.at[y, k], loc.at[NC])
    loads = {}
    for what, n in steps:
        if what in "fg" and n not in loads:
            loads[n] = local_copies(n)
            for cp in loads[n]:
                cp.start()
        if what in "cC" and NC not in loads:
            c0load.start()
            loads[NC] = [c0load]
    pl.semaphore_wait(barrier, 3)

    lane = lax.broadcasted_iota(jnp.int32, (8, W), 1)
    grp = lane // 16

    def turn(v):
        return jnp.concatenate([v[:, W // 2:], v[:, :W // 2]], axis=1)

    def loaded(c):
        copies = loads.pop(c, [])
        for cp in copies:
            cp.wait()
        if copies and c < NC and CHUNKS[c] is None:
            h = c // 4
            for g in range(3):
                for m in range(4):
                    v = jnp.where(lane < W // 2, raw[h, 2 * g, m], turn(raw[h, 2 * g + 1, m]))
                    ld[h, y, k, 6 + g, m, x] = v

    def own_first(c):
        loaded(c)
        put(c, NF, y, x, first(c))
        put(c, SO, y, x, sid)

    def own_second(c):
        loaded(c)
        put(c, NG, y, x, second(c))

    def cref(n, q, p):
        s, m0, m1 = CP[n]
        return c0.at[q, p, 8 * s + m0:8 * s + m1]

    def cput(n, kind, q, dev):
        ref = cref(n, q, k)
        return remote(ref, ref, snd.at[0], crcv.at[n, kind], dev)

    def cgot(n, kind, q, p):
        ref = cref(n, q, p)
        remote(ref, ref, snd.at[0], crcv.at[n, kind], sid).wait_recv()

    def clear():
        xa[...] = jnp.zeros(xa.shape, F32)
        xb[...] = jnp.zeros(xb.shape, F32)
        zz[...] = jnp.zeros(zz.shape, F32)

    def serve_f(c):
        q, xs = from_first(c, k)
        got(c, NF, q, k, xs)
        put(c, ND, q, xs, second(c))
        put(c, SF, q, xs, sid)

    def serve_g(c):
        q, xs = from_second(c, k)
        got(c, NG, q, k, xs)
        put(c, SG, q, xs, sid)

    def serve_d(c):
        got(c, ND, oy, k, ox)
        put(c, SD, oy, ox, sid)

    def ready(c):
        got(c, SO, y, ok, x)
        q, xs = from_first(c, ok)
        got(c, SF, q, ok, xs)
        q, xs = from_second(c, ok)
        got(c, SG, q, ok, xs)
        got(c, SD, oy, ok, ox)

    G6 = 3
    lane48 = lax.broadcasted_iota(jnp.int32, (8 * G6, W), 1)
    sub48 = lax.broadcasted_iota(jnp.int32, (8 * G6, W), 0) % 8
    base48 = (lane48 // 16) * 16
    def rowcast(v, e):
        v3 = v.reshape(G6, 8, W)[:, e:e + 1, :]
        return jnp.broadcast_to(v3, (G6, 8, W)).reshape(8 * G6, W)

    def dl(half, g, q, p, m, sg):
        if m >= 4:
            return ld[half, q, p, 2 * g + k, m - 4, sg]
        v = ld[half, q, p, 6 + g, m, sg]
        return jnp.where(k == 1, turn(v), v)

    def substitute(half):
        sub = {}
        for p in range(2):
            for sg in range(2):
                for q in range(2):
                    rows = []
                    for g in range(G6):
                        v = jnp.zeros((8, W), F32)
                        for m in range(8):
                            v = jnp.where(grp == m, dl(half, g, q, p, m, sg), v)
                        rows.append(v)
                    sub[2 * sg + p, q] = jnp.concatenate(rows, axis=0)
        yv = {}
        for be in range(4):
            for q in range(2):
                if be % 2 == q:
                    yv[be, q] = jnp.where(lane48 % 16 == 8 * (be // 2) + sub48, 1.0, 0.0).astype(F32)
                else:
                    yv[be, q] = jnp.zeros((8 * G6, W), F32)

        for be in range(4):
            for e in range(8):
                idx = base48 + (8 * (be // 2) + e)
                gs = {b2: jnp.take_along_axis(sub[b2, be % 2], idx, axis=1, mode="promise_in_bounds")
                      for b2 in range(be, 4)}
                rinv = 1.0 / rowcast(gs[be], e)
                for q in range(2):
                    piv = rowcast(yv[be, q], e) * rinv
                    for b2 in range(be, 4):
                        new = yv[b2, q] - gs[b2] * piv
                        if b2 == be:
                            new = jnp.where(sub48 > e, new, jnp.where(sub48 == e, piv, yv[b2, q]))
                        yv[b2, q] = new
        for be in range(4):
            for q in range(2):
                ys[be, q] = yv[be, q].reshape(G6, 8, W)

    lane256 = lax.broadcasted_iota(jnp.int32, (8, T2), 1) % W

    def invert(half, count=G6):
        dd, ll = [], []
        for n in range(count):
            g = n
            rows = []
            for p in range(2):
                for m in range(8):
                    for sg in range(2):
                        parts = [jnp.where(grp == m, ys[2 * sg + p, q, g], 0.0) for q in range(2)]
                        rows.append(jnp.concatenate(parts, axis=1))
            dd.append(rows)
            ll.append([jnp.concatenate([dl(half, g, q, p, m, sg) for q in range(2)], axis=1)
                       for p in range(2) for m in range(8) for sg in range(2)])
        for h8 in (2, 4, 8):
            odd = [b for b in range(32) if (b % 16) // h8 % 2 == 1]
            zero = jnp.zeros((8, T2), F32)
            tds = []
            for n in range(count):
                mo = [jnp.where(lane256 // (8 * h8) == (b % 16) // h8 - 1, ll[n][b], 0.0) for b in odd]
                tds.append(dot(jnp.concatenate(mo, axis=0), jnp.concatenate(dd[n], axis=0)))
            for n in range(count):
                tfull = [zero] * 32
                for o, b in enumerate(odd):
                    tfull[b] = tds[n][8 * o:8 * o + 8]
                xo = dot(jnp.concatenate([dd[n][b] for b in odd], axis=0), jnp.concatenate(tfull, axis=0))
                for o, b in enumerate(odd):
                    dd[n][b] = dd[n][b] - xo[8 * o:8 * o + 8]
        for n in range(count):
            db[G6 * half + n, k] = jnp.concatenate(dd[n], axis=0)
        dbcopy(half, k).start()

    def dbcopy(half, kk):
        ref = db.at[G6 * half:G6 * half + G6, kk]
        return remote(ref, ref, snd.at[0], misc_r.at[half], sid)

    def ltile(t):
        return jnp.concatenate([lt[t, q].reshape(T2, W) for q in range(2)], axis=1)

    need = [0, 1, 1, 0, 0, 1]

    def place_a(i):
        @pl.when(k == need[i])
        def _():
            t = i // 2
            d = db[i // 2, i % 2, :, pl.ds(pl.multiple_of(y * W, W), W)]
            xa[i, :, :, :, :, W * t:W * t + W] = d.reshape(2, 8, 2, 8, W)

    def step_a(i):
        for j in range(i):
            n = W * (j // 2 + 1)
            d = dot(ltile(TIDX[i, j]), xa[j, :, :, :, :, 0:n].reshape(T2, n))
            n0 = 0 if j == 0 else W * ((j - 1) // 2 + 1)
            if n0:
                acc[:, 0:n0] = acc[:, 0:n0] + d[:, 0:n0]
            if n > n0:
                acc[:, n0:n] = d[:, n0:n]
        n = W * ((i + 1) // 2)
        r = -dot(db[i // 2, i % 2], acc[:, 0:n])
        xa[i, :, :, :, :, 0:n] = r.reshape(2, 8, 2, 8, n)
        place_a(i)

    def place_b(i):
        d = db[3 + i // 2, i % 2, :, pl.ds(pl.multiple_of(k * W, W), W)]
        xb[i, :, :, :, :, W * i:W * i + W] = d.reshape(2, 8, 2, 8, W)

    def step_b(i):
        for j in range(i):
            n = W * (j + 1)
            d = dot(ltile(TIDX[i + 6, j + 6]), xb[j, :, :, :, :, 0:n].reshape(T2, n))
            if j:
                acc[:, 0:n - W] = acc[:, 0:n - W] + d[:, 0:n - W]
            acc[:, n - W:n] = d[:, n - W:n]
        n = W * i
        r = -dot(db[3 + i // 2, i % 2], acc[:, 0:n])
        xb[i, :, :, :, :, 0:n] = r.reshape(2, 8, 2, 8, n)
        place_b(i)

    outs = []

    def put_out(src, dst):
        cp = pltpu.make_async_copy(src, dst, osem.at[0])
        cp.start()
        outs.append(cp)

    def jcol(t, kk):
        return [kk, 3 - kk, 4 + kk][t]

    def lanes(t, kk):
        return pl.ds(pl.multiple_of(W * jcol(t, kk), W), W)

    oacopy = remote(xa.at[:, ok, :, x, :, :], oa, snd.at[0], misc_r.at[2], sid)

    def finish_a():
        oacopy.start()
        for i in range(6):
            put_out(zz, out.at[i, :, :, HW:2 * HW])
        for t in range(3):
            put_out(xa.at[:, k, :, x, :, W * t:W * t + W], out.at[0:6, :, :, lanes(t, k)])

    def finish_oa():
        remote(oa, oa, snd.at[0], misc_r.at[2], sid).wait_recv()
        for t in range(3):
            put_out(oa.at[:, :, :, W * t:W * t + W], out.at[0:6, :, :, lanes(t, ok)])

    def bxcopy(i, kk):
        return remote(xb.at[i, :, :, x, :, :], bx.at[kk, i], snd.at[0], brcv.at[i], sid)

    def bxlocal(i):
        return pltpu.make_async_copy(xb.at[i, :, :, x, :, :], bx.at[k, i], bloc.at[i])

    def send_b(i):
        bxcopy(i, k).start()
        bxlocal(i).start()

    def get_b(i):
        bxlocal(i).wait()
        bxcopy(i, ok).wait_recv()
        put_out(bx.at[y, i, k], out.at[6 + i, :, :, HW:2 * HW])

    def tcopy(n, xs):
        s, m0, m1 = CP[n]
        ref = tt.at[s, :, m0:m1, xs, :, :]
        return remote(ref, ref, snd.at[0], trcv.at[n], xid)

    def serve_c(n):
        cgot(n, 0, oy, k)
        cput(n, 2, oy, sid).start()

    def do_t(h):
        group = TG[h]
        for n in group:
            cgot(n, 1, y, ok)
            cgot(n, 2, oy, ok)
        lo = 8 * CP[group[0]][0] + CP[group[0]][1]
        hi = 8 * CP[group[-1]][0] + CP[group[-1]][2]
        g = 8 * (hi - lo)
        for u in range(3):
            w = W * (u + 1)
            parts = []
            for j in (2 * u, 2 * u + 1):
                for q in range(2):
                    parts.append(c0[q, :, lo:hi, :, W * j:W * j + W].reshape(2 * g, W))
            rhs = jnp.concatenate([xa[2 * u + e, :, :, :, :, 0:w].reshape(T2, w) for e in range(2)], axis=0)
            d = dot(jnp.concatenate(parts, axis=1), rhs)
            if u:
                acc[0:2 * g, 0:w - W] = acc[0:2 * g, 0:w - W] + d[:, 0:w - W]
            acc[0:2 * g, w - W:w] = d[:, w - W:w]
        for n in group:
            s, m0, m1 = CP[n]
            at = 8 * (8 * s + m0 - lo)
            size = 8 * (m1 - m0)
            for p in range(2):
                r = acc[p * g + at:p * g + at + size, 0:JW]
                tt[s, p, m0:m1, x, :, :] = r.reshape(m1 - m0, 8, JW)
            tcopy(n, x).start()

    def tgot(s):
        for n in range(NP):
            if CP[n][0] == s:
                tcopy(n, ox).wait_recv()

    def bpart(s, count, u, nu):
        parts = []
        for e in range(nu):
            ln = pl.ds(pl.multiple_of((u + e) * W, W), W)
            for q in range(2):
                parts.append(bx[q, s:s + count, :, :, :, ln].reshape(count * W, W))
        rhs = jnp.concatenate([tt[u + e].reshape(T2, JW) for e in range(nu)], axis=0)
        return dot(jnp.concatenate(parts, axis=1), rhs)

    def do_p(a):
        for s in (2 * a, 2 * a + 1):
            get_b(s)

        def body(it, carry):
            accx[...] = accx[...] - bpart(2 * a, 2, 2 * it, 2)
            return carry

        if a > 1:
            accx[...] = jnp.zeros((T2, JW), F32)
            lax.fori_loop(0, a, body, 0)
        elif a == 1:
            accx[...] = -bpart(2, 2, 0, 2)

    def do_x(s):
        tgot(s)
        if s == 0:
            accx[...] = -bpart(0, 2, 0, 1)
        elif s % 2 == 0:
            accx[...] = accx[...] - bpart(s, 2, s, 1)
        else:
            accx[W:, :] = accx[W:, :] - bpart(s, 1, s, 1)
        at = W * (s % 2)
        xc[s] = accx[at:at + W, :].reshape(2, 8, 8, JW)
        remote(xc.at[s, ok], oc.at[s], snd.at[0], orcv.at[s], sid).start()
        for t in range(3):
            put_out(xc.at[s, k, :, :, W * t:W * t + W], out.at[6 + s, :, :, lanes(t, k)])

    def finish_x(s):
        remote(oc.at[s], oc.at[s], snd.at[0], orcv.at[s], sid).wait_recv()
        for t in range(3):
            put_out(oc.at[s, :, :, W * t:W * t + W], out.at[6 + s, :, :, lanes(t, ok)])

    def inv(half):
        substitute(half)
        invert(half)

    def get_d(half):
        dbcopy(half, ok).wait_recv()
        (place_b if half else place_a)(0)

    def do_b(i):
        step_b(i)
        send_b(i)

    def csend(n):
        loaded(NC)
        cput(n, 0, y, yid).start()

    def csib(n):
        loaded(NC)
        cput(n, 1, y, sid).start()

    run = {"f": own_first, "g": own_second, "F": serve_f, "G": serve_g, "D": serve_d, "R": ready, "I": inv,
           "Q": get_d, "A": step_a, "B": do_b, "S": send_b, "C": csend, "c": csib, "V": serve_c, "T": do_t,
           "X": do_x, "P": do_p, "Y": finish_x, "a": lambda _: finish_a(), "o": lambda _: finish_oa()}
    cleared = False
    for what, n in steps:
        if what in "FGDR" and not cleared:
            clear()
            cleared = True
        with jax.named_scope(f"{what}{n}"):
            run[what](n)

    for cp in started:
        cp.wait_send()
    for n in range(NP):
        cput(n, 0, y, yid).wait_send()
        cput(n, 1, y, sid).wait_send()
        cput(n, 2, oy, sid).wait_send()
        tcopy(n, x).wait_send()
    for s in range(6):
        bxcopy(s, k).wait_send()
        remote(xc.at[s, ok], oc.at[s], snd.at[0], orcv.at[s], sid).wait_send()
    dbcopy(0, k).wait_send()
    dbcopy(1, k).wait_send()
    oacopy.wait_send()
    for cp in outs:
        cp.wait()


def solution(mesh):
    spec = P(("batch", "row"), "col")
    vm = lambda *shape: pltpu.VMEM(shape, F32)
    dma = lambda *shape: pltpu.SemaphoreType.DMA(shape)

    def body(local_l):
        got = pl.pallas_call(
            kernel,
            name="tri_inverse",
            out_shape=jax.ShapeDtypeStruct((12, 8, 8, 1536), F32),
            in_specs=[pl.BlockSpec(memory_space=pl.ANY)],
            out_specs=pl.BlockSpec(memory_space=pl.ANY),
            scratch_shapes=[
                vm(30, 2, 2, 8, 2, 8, W),
                vm(2, 2, 2, 9, 4, 2, 8, W),
                vm(2, 6, 4, 8, W),
                vm(2, 2, 48, 8, HW),
                vm(6, 2, 8, 2, 8, JW),
                vm(6, 2, 8, 2, 8, HW),
                vm(2, 6, 2, 8, 8, HW),
                vm(6, 2, 8, 2, 8, JW),
                vm(6, 2, T2, T2),
                vm(6, 8, 8, JW),
                vm(6, 2, 8, 8, JW),
                vm(6, 8, 8, JW),
                vm(8, 8, HW),
                vm(T2, HW),
                vm(T2, JW),
                vm(4, 2, 3, 8, W),
                dma(NC + 1), dma(1), dma(NC, 7), dma(NP, 3), dma(NP), dma(6), dma(6), dma(6), dma(3), dma(1),
            ],
            compiler_params=pltpu.CompilerParams(
                collective_id=0, has_side_effects=True, vmem_limit_bytes=47 * 2**20),
        )(local_l.reshape(96, 8, 1536))
        return got.reshape(HW, 1536)

    return jax.shard_map(body, mesh=mesh, in_specs=(spec,), out_specs=spec, check_vma=False)
```

```python
import functools

import jax
import jax.numpy as jnp
from jax import lax
from jax.experimental import pallas as pl
from jax.experimental.pallas import tpu as pltpu
from jax.sharding import PartitionSpec as P

MESH = pl.DeviceIdType.MESH
F32 = jnp.float32

OFF_A = [(i, j) for i in range(1, 6) for j in range(i)]
OFF_B = [(i + 6, j + 6) for i in range(1, 6) for j in range(i)]
TILES = OFF_A + OFF_B
TIDX = {ij: t for t, ij in enumerate(TILES)}
CHUNKS = [None, (0, 6), (6, 10), (10, 15), None, (15, 21), (21, 25), (25, 30)]
NC = len(CHUNKS)
NF, NG, ND, SIB = range(4)
CP = [(0, 0, 8), (1, 0, 8), (2, 0, 8), (3, 0, 8), (4, 0, 8), (5, 0, 4), (5, 4, 8)]
NP = len(CP)
TG = [(0, 1), (2, 3), (4,), (5,), (6,)]
ORDER = [
    "f1 f4 f0 f2", "g0 c3 C0 F4", "g1 F0 c2 G0", "g3 f3 g2 g4", "G1 D0 f5 c5", "R0 F1 c4 F2",
    "g5 I0 D4 F3", "G4 D1 R4 c0", "g6 c1 I1 Q0", "G2 f6 C1 V0", "R1 D2 F5 Q1", "G5 G3 C2 A1",
    "A2 A3 R2 D3", "R3 f7 S0 c6", "C3 F6 C4 G6", "A4 V1 A5 D5", "T0 V2 R5 F7", "a0 C5 B1 D6",
    "B2 V3 T1 V4", "B3 P0 R6 g7", "X0 T2 X1 B4", "Y1 P1 D7 C6", "V5 G7 X2 T3", "R7 V6 B5 Y2",
    "o0 T4 X3 P2", "X4 X5 Y0 Y4", "Y3 Y5",
]
MODES = [2, 2, 3, 1, 1, 2, 2, 3]
W, T2, JW, HW = 128, 256, 384, 768
QW, HALF, SH = 32, 64, 24
TWO = range(2)


def dot(a, b):
    return jnp.dot(a, b, precision=lax.Precision.HIGHEST, preferred_element_type=F32)


def kernel(l_hbm, out, lt, ld, raw, c0, xa, xb, bx, tt, db, oa, xc, oc, zz, acc, accx, ys,
           loc, snd, rcv, crcv, trcv, orcv, brcv, bloc, misc_r, osem):
    row = lax.axis_index("row")
    y = lax.axis_index("col")
    x = row // 2
    k = row % 2
    ox, ok, oy = 1 - x, 1 - k, 1 - y
    sid = {"row": 2 * x + ok, "col": y}
    xid = {"row": 2 * ox + k, "col": y}
    yid = {"row": row, "col": oy}

    def way(c, core):
        return (core, 1 - core, 1, 0)[MODES[c]]

    def first(c):
        v = way(c, k)
        return {"row": row + (1 - v) * 2 * (1 - 2 * x), "col": y + v * (1 - 2 * y)}

    def second(c):
        v = 1 - way(c, k)
        return {"row": row + (1 - v) * 2 * (1 - 2 * x), "col": y + v * (1 - 2 * y)}

    def from_first(c, core):
        v = way(c, core)
        return y + v * (1 - 2 * y), x + (1 - v) * (1 - 2 * x)

    def from_second(c, core):
        v = 1 - way(c, core)
        return y + v * (1 - 2 * y), x + (1 - v) * (1 - 2 * x)

    started = []

    def remote(src, dst, ss, rs, dev):
        cp = pltpu.make_async_remote_copy(src_ref=src, dst_ref=dst, send_sem=ss, recv_sem=rs,
                                          device_id=dev, device_id_type=MESH)
        return cp

    def piece(c, q, p, xs):
        if CHUNKS[c] is None:
            return ld.at[c // 4, q, p, :, xs, :, :]
        a, b = CHUNKS[c]
        return lt.at[a:b, q, p, :, xs, :, :]

    def put(c, kind, q, xs, dev):
        ref = piece(c, q, k, xs)
        cp = remote(ref, ref, snd.at[0], rcv.at[c, kind], dev)
        cp.start()
        started.append(cp)

    def got(c, kind, q, p, xs):
        ref = piece(c, q, p, xs)
        remote(ref, ref, snd.at[0], rcv.at[c, kind], sid).wait_recv()

    def local_copies(c):
        if CHUNKS[c] is None:
            h = c // 4
            low, high = [], []
            for n in range(6):
                i = 6 * h + n
                cols = slice(W * i, W * i + W)
                low.append(pltpu.make_async_copy(l_hbm.at[8 * i:8 * i + 6, :, cols], raw.at[h, n], loc.at[c]))
                high.append(pltpu.make_async_copy(l_hbm.at[8 * i + 6:8 * i + 8, :, cols],
                                                  ld.at[h, y, k, 4 * n + 2:4 * n + 4, x, :, :], loc.at[c]))
            return low + high
        a, b = CHUNKS[c]
        return [pltpu.make_async_copy(l_hbm.at[8 * i:8 * i + 8, :, W * j:W * j + W],
                                      lt.at[a + n, y, k, :, x, :, :], loc.at[c])
                for n, (i, j) in enumerate(TILES[a:b])]

    barrier = pltpu.get_barrier_semaphore()
    for dev in (xid, yid, sid):
        pl.semaphore_signal(barrier, inc=1, device_id=dev, device_id_type=MESH)
    steps = [(name[0], int(name[1:] or 0)) for group in ORDER for name in group.split()]
    c0load = pltpu.make_async_copy(l_hbm.at[48:96, :, 0:HW], c0.at[y, k], loc.at[NC])
    loads = {}
    for what, n in steps:
        if what in "fg" and n not in loads:
            loads[n] = local_copies(n)
            for cp in loads[n]:
                cp.start()
        if what in "cC" and NC not in loads:
            c0load.start()
            loads[NC] = [c0load]
    pl.semaphore_wait(barrier, 3)

    lane = lax.broadcasted_iota(jnp.int32, (8, W), 1)
    grp = lane // 16

    def turn(v, by):
        return jnp.concatenate([v[:, by:], v[:, :by]], axis=1)

    def loaded(c):
        copies = loads.pop(c, [])
        for cp in copies:
            cp.wait()
        if copies and c < NC and CHUNKS[c] is None:
            h = c // 4
            for n in range(6):
                for e in TWO:
                    v = jnp.where(lane < W - QW, raw[h, n, 4 + e], turn(raw[h, n, e], QW))
                    ld[h, y, k, 4 * n + e, x] = v
            for g in range(3):
                for e in TWO:
                    v = jnp.where(lane < HALF, raw[h, 2 * g, 2 + e], turn(raw[h, 2 * g + 1, 2 + e], HALF))
                    ld[h, y, k, SH + 2 * g + e, x] = v

    def own_first(c):
        loaded(c)
        put(c, NF, y, x, first(c))
        put(c, SIB, y, x, sid)

    def own_second(c):
        loaded(c)
        put(c, NG, y, x, second(c))

    def cref(n, q, p):
        s, m0, m1 = CP[n]
        return c0.at[q, p, 8 * s + m0:8 * s + m1]

    def cput(n, kind, q, dev):
        ref = cref(n, q, k)
        return remote(ref, ref, snd.at[0], crcv.at[n, kind], dev)

    def cgot(n, kind, q, p):
        ref = cref(n, q, p)
        remote(ref, ref, snd.at[0], crcv.at[n, kind], sid).wait_recv()

    def clear():
        xa[...] = jnp.zeros(xa.shape, F32)
        xb[...] = jnp.zeros(xb.shape, F32)
        zz[...] = jnp.zeros(zz.shape, F32)

    def serve_f(c):
        q, xs = from_first(c, k)
        got(c, NF, q, k, xs)
        put(c, ND, q, xs, second(c))
        put(c, SIB, q, xs, sid)

    def serve_g(c):
        q, xs = from_second(c, k)
        got(c, NG, q, k, xs)
        put(c, SIB, q, xs, sid)

    def serve_d(c):
        got(c, ND, oy, k, ox)
        put(c, SIB, oy, ox, sid)

    def ready(c):
        if CHUNKS[c] is None:
            ref = ld.at[c // 4, :, ok]
        else:
            lo, hi = CHUNKS[c]
            ref = lt.at[lo:hi, :, ok]
        remote(ref, ref, snd.at[0], rcv.at[c, SIB], sid).wait_recv()

    G6 = 3
    lane48 = lax.broadcasted_iota(jnp.int32, (8 * G6, W), 1)
    sub48 = lax.broadcasted_iota(jnp.int32, (8 * G6, W), 0) % 8
    base48 = (lane48 // 16) * 16
    def rowcast(v, e):
        v3 = v.reshape(G6, 8, W)[:, e:e + 1, :]
        return jnp.broadcast_to(v3, (G6, 8, W)).reshape(8 * G6, W)

    def dl(half, g, q, p, m, sg):
        at = 4 * (2 * g + k)
        if m >= 4:
            return ld[half, q, p, at + m - 4, sg]
        if m < 2:
            return turn(ld[half, q, p, at + m, sg], W - QW)
        v = ld[half, q, p, SH + 2 * g + m - 2, sg]
        return jnp.where(k == 1, turn(v, HALF), v)

    def substitute(half):
        sub = {}
        for p in TWO:
            for sg in TWO:
                for q in TWO:
                    rows = []
                    for g in range(G6):
                        v = jnp.zeros((8, W), F32)
                        for m in range(8):
                            v = jnp.where(grp == m, dl(half, g, q, p, m, sg), v)
                        rows.append(v)
                    sub[2 * sg + p, q] = jnp.concatenate(rows, axis=0)
        yv = {}
        for be in range(4):
            for q in TWO:
                if be % 2 == q:
                    yv[be, q] = jnp.where(lane48 % 16 == 8 * (be // 2) + sub48, 1.0, 0.0).astype(F32)
                else:
                    yv[be, q] = jnp.zeros((8 * G6, W), F32)

        for be in range(4):
            for e in range(8):
                idx = base48 + (8 * (be // 2) + e)
                gs = {b2: jnp.take_along_axis(sub[b2, be % 2], idx, axis=1, mode="promise_in_bounds")
                      for b2 in range(be, 4)}
                rinv = 1.0 / rowcast(gs[be], e)
                for q in TWO:
                    piv = rowcast(yv[be, q], e) * rinv
                    for b2 in range(be, 4):
                        new = yv[b2, q] - gs[b2] * piv
                        if b2 == be:
                            new = jnp.where(sub48 > e, new, jnp.where(sub48 == e, piv, yv[b2, q]))
                        yv[b2, q] = new
        for be in range(4):
            for q in TWO:
                ys[be, q] = yv[be, q].reshape(G6, 8, W)

    lane256 = lax.broadcasted_iota(jnp.int32, (8, T2), 1) % W

    def invert(half, count=G6):
        dd, ll = [], []
        for n in range(count):
            g = n
            rows = []
            for p in TWO:
                for m in range(8):
                    for sg in TWO:
                        parts = [jnp.where(grp == m, ys[2 * sg + p, q, g], 0.0) for q in TWO]
                        rows.append(jnp.concatenate(parts, axis=1))
            dd.append(rows)
            ll.append([jnp.concatenate([dl(half, g, q, p, m, sg) for q in TWO], axis=1)
                       for p in TWO for m in range(8) for sg in TWO])
        for h8 in (2, 4, 8):
            odd = [b for b in range(32) if (b % 16) // h8 % 2 == 1]
            zero = jnp.zeros((8, T2), F32)
            tds = []
            for n in range(count):
                mo = [jnp.where(lane256 // (8 * h8) == (b % 16) // h8 - 1, ll[n][b], 0.0) for b in odd]
                tds.append(dot(jnp.concatenate(mo, axis=0), jnp.concatenate(dd[n], axis=0)))
            for n in range(count):
                tfull = [zero] * 32
                for o, b in enumerate(odd):
                    tfull[b] = tds[n][8 * o:8 * o + 8]
                xo = dot(jnp.concatenate([dd[n][b] for b in odd], axis=0), jnp.concatenate(tfull, axis=0))
                for o, b in enumerate(odd):
                    dd[n][b] = dd[n][b] - xo[8 * o:8 * o + 8]
        for n in range(count):
            db[G6 * half + n, k] = jnp.concatenate(dd[n], axis=0)
        dbcopy(half, k).start()

    def dbcopy(half, kk):
        ref = db.at[G6 * half:G6 * half + G6, kk]
        return remote(ref, ref, snd.at[0], misc_r.at[half], sid)

    def ltile(t):
        return jnp.concatenate([lt[t, q].reshape(T2, W) for q in TWO], axis=1)

    need = [0, 1, 1, 0, 0, 1]

    def place_a(i):
        @pl.when(k == need[i])
        def _():
            t = i // 2
            d = db[i // 2, i % 2, :, pl.ds(pl.multiple_of(y * W, W), W)]
            xa[i, :, :, :, :, W * t:W * t + W] = d.reshape(2, 8, 2, 8, W)

    def step_a(i):
        for j in range(i):
            n = W * (j // 2 + 1)
            d = dot(ltile(TIDX[i, j]), xa[j, :, :, :, :, 0:n].reshape(T2, n))
            n0 = 0 if j == 0 else W * ((j - 1) // 2 + 1)
            if n0:
                acc[:, 0:n0] = acc[:, 0:n0] + d[:, 0:n0]
            if n > n0:
                acc[:, n0:n] = d[:, n0:n]
        n = W * ((i + 1) // 2)
        r = -dot(db[i // 2, i % 2], acc[:, 0:n])
        xa[i, :, :, :, :, 0:n] = r.reshape(2, 8, 2, 8, n)
        place_a(i)

    def place_b(i):
        d = db[3 + i // 2, i % 2, :, pl.ds(pl.multiple_of(k * W, W), W)]
        xb[i, :, :, :, :, W * i:W * i + W] = d.reshape(2, 8, 2, 8, W)

    def step_b(i):
        for j in range(i):
            n = W * (j + 1)
            d = dot(ltile(TIDX[i + 6, j + 6]), xb[j, :, :, :, :, 0:n].reshape(T2, n))
            if j:
                acc[:, 0:n - W] = acc[:, 0:n - W] + d[:, 0:n - W]
            acc[:, n - W:n] = d[:, n - W:n]
        n = W * i
        r = -dot(db[3 + i // 2, i % 2], acc[:, 0:n])
        xb[i, :, :, :, :, 0:n] = r.reshape(2, 8, 2, 8, n)
        place_b(i)

    outs = []

    def put_out(src, dst):
        cp = pltpu.make_async_copy(src, dst, osem.at[0])
        cp.start()
        outs.append(cp)

    def jcol(t, kk):
        return [kk, 3 - kk, 4 + kk][t]

    def lanes(t, kk):
        return pl.ds(pl.multiple_of(W * jcol(t, kk), W), W)

    oacopy = remote(xa.at[:, ok, :, x, :, :], oa, snd.at[0], misc_r.at[2], sid)

    def finish_a():
        oacopy.start()
        for i in range(6):
            put_out(zz, out.at[i, :, :, HW:2 * HW])
        for t in range(3):
            put_out(xa.at[:, k, :, x, :, W * t:W * t + W], out.at[0:6, :, :, lanes(t, k)])

    def finish_oa():
        remote(oa, oa, snd.at[0], misc_r.at[2], sid).wait_recv()
        for t in range(3):
            put_out(oa.at[:, :, :, W * t:W * t + W], out.at[0:6, :, :, lanes(t, ok)])

    def bxcopy(i, kk):
        return remote(xb.at[i, :, :, x, :, :], bx.at[kk, i], snd.at[0], brcv.at[i], sid)

    def bxlocal(i):
        return pltpu.make_async_copy(xb.at[i, :, :, x, :, :], bx.at[k, i], bloc.at[i])

    def send_b(i):
        bxcopy(i, k).start()
        bxlocal(i).start()

    def get_b(i):
        bxlocal(i).wait()
        bxcopy(i, ok).wait_recv()
        put_out(bx.at[y, i, k], out.at[6 + i, :, :, HW:2 * HW])

    def tcopy(n, xs):
        s, m0, m1 = CP[n]
        ref = tt.at[s, :, m0:m1, xs, :, :]
        return remote(ref, ref, snd.at[0], trcv.at[n], xid)

    def serve_c(n):
        cgot(n, 0, oy, k)
        cput(n, 1, oy, sid).start()

    def do_t(h):
        group = TG[h]
        for n in group:
            s, m0, m1 = CP[n]
            both = c0.at[:, ok, 8 * s + m0:8 * s + m1]
            remote(both, both, snd.at[0], crcv.at[n, 1], sid).wait_recv()
        lo = 8 * CP[group[0]][0] + CP[group[0]][1]
        hi = 8 * CP[group[-1]][0] + CP[group[-1]][2]
        g = 8 * (hi - lo)
        for u in range(3):
            w = W * (u + 1)
            parts = []
            for j in (2 * u, 2 * u + 1):
                for q in TWO:
                    parts.append(c0[q, :, lo:hi, :, W * j:W * j + W].reshape(2 * g, W))
            rhs = jnp.concatenate([xa[2 * u + e, :, :, :, :, 0:w].reshape(T2, w) for e in TWO], axis=0)
            d = dot(jnp.concatenate(parts, axis=1), rhs)
            if u:
                acc[0:2 * g, 0:w - W] = acc[0:2 * g, 0:w - W] + d[:, 0:w - W]
            acc[0:2 * g, w - W:w] = d[:, w - W:w]
        for n in group:
            s, m0, m1 = CP[n]
            at = 8 * (8 * s + m0 - lo)
            size = 8 * (m1 - m0)
            for p in TWO:
                r = acc[p * g + at:p * g + at + size, 0:JW]
                tt[s, p, m0:m1, x, :, :] = r.reshape(m1 - m0, 8, JW)
            tcopy(n, x).start()

    def tgot(s):
        for n in range(NP):
            if CP[n][0] == s:
                tcopy(n, ox).wait_recv()

    def bpart(s, count, u, nu):
        parts = []
        for e in range(nu):
            ln = pl.ds(pl.multiple_of((u + e) * W, W), W)
            for q in TWO:
                parts.append(bx[q, s:s + count, :, :, :, ln].reshape(count * W, W))
        rhs = jnp.concatenate([tt[u + e].reshape(T2, JW) for e in range(nu)], axis=0)
        return dot(jnp.concatenate(parts, axis=1), rhs)

    def do_p(a):
        for s in (2 * a, 2 * a + 1):
            get_b(s)

        def body(it, carry):
            accx[...] = accx[...] - bpart(2 * a, 2, 2 * it, 2)
            return carry

        if a > 1:
            accx[...] = jnp.zeros((T2, JW), F32)
            lax.fori_loop(0, a, body, 0)
        elif a == 1:
            accx[...] = -bpart(2, 2, 0, 2)

    def do_x(s):
        tgot(s)
        if s == 0:
            accx[...] = -bpart(0, 2, 0, 1)
        elif s % 2 == 0:
            accx[...] = accx[...] - bpart(s, 2, s, 1)
        else:
            accx[W:, :] = accx[W:, :] - bpart(s, 1, s, 1)
        at = W * (s % 2)
        xc[s] = accx[at:at + W, :].reshape(2, 8, 8, JW)
        remote(xc.at[s, ok], oc.at[s], snd.at[0], orcv.at[s], sid).start()
        for t in range(3):
            put_out(xc.at[s, k, :, :, W * t:W * t + W], out.at[6 + s, :, :, lanes(t, k)])

    def finish_x(s):
        remote(oc.at[s], oc.at[s], snd.at[0], orcv.at[s], sid).wait_recv()
        for t in range(3):
            put_out(oc.at[s, :, :, W * t:W * t + W], out.at[6 + s, :, :, lanes(t, ok)])

    def inv(half):
        substitute(half)
        invert(half)

    def get_d(half):
        dbcopy(half, ok).wait_recv()
        (place_b if half else place_a)(0)

    def do_b(i):
        step_b(i)
        send_b(i)

    def csend(n):
        loaded(NC)
        cput(n, 0, y, yid).start()

    def csib(n):
        loaded(NC)
        cput(n, 1, y, sid).start()

    run = {"f": own_first, "g": own_second, "F": serve_f, "G": serve_g, "D": serve_d, "R": ready, "I": inv,
           "Q": get_d, "A": step_a, "B": do_b, "S": send_b, "C": csend, "c": csib, "V": serve_c, "T": do_t,
           "X": do_x, "P": do_p, "Y": finish_x, "a": lambda _: finish_a(), "o": lambda _: finish_oa()}
    cleared = False
    for what, n in steps:
        if what in "FGDR" and not cleared:
            clear()
            cleared = True
        with jax.named_scope(f"{what}{n}"):
            run[what](n)

    for cp in started:
        cp.wait_send()
    for n in range(NP):
        cput(n, 0, y, yid).wait_send()
        cput(n, 1, y, sid).wait_send()
        cput(n, 1, oy, sid).wait_send()
        tcopy(n, x).wait_send()
    for s in range(6):
        bxcopy(s, k).wait_send()
        remote(xc.at[s, ok], oc.at[s], snd.at[0], orcv.at[s], sid).wait_send()
    dbcopy(0, k).wait_send()
    dbcopy(1, k).wait_send()
    oacopy.wait_send()
    for cp in outs:
        cp.wait()


def solution(mesh):
    spec = P(("batch", "row"), "col")
    vm = lambda *shape: pltpu.VMEM(shape, F32)
    dma = lambda *shape: pltpu.SemaphoreType.DMA(shape)

    def body(local_l):
        got = pl.pallas_call(
            kernel,
            name="tri_inverse",
            out_shape=jax.ShapeDtypeStruct((12, 8, 8, 1536), F32),
            in_specs=[pl.BlockSpec(memory_space=pl.ANY)],
            out_specs=pl.BlockSpec(memory_space=pl.ANY),
            scratch_shapes=[
                vm(30, 2, 2, 8, 2, 8, W),
                vm(2, 2, 2, 30, 2, 8, W),
                vm(2, 6, 6, 8, W),
                vm(2, 2, 48, 8, HW),
                vm(6, 2, 8, 2, 8, JW),
                vm(6, 2, 8, 2, 8, HW),
                vm(2, 6, 2, 8, 8, HW),
                vm(6, 2, 8, 2, 8, JW),
                vm(6, 2, T2, T2),
                vm(6, 8, 8, JW),
                vm(6, 2, 8, 8, JW),
                vm(6, 8, 8, JW),
                vm(8, 8, HW),
                vm(T2, HW),
                vm(T2, JW),
                vm(4, 2, 3, 8, W),
                dma(NC + 1), dma(1), dma(NC, 4), dma(NP, 2), dma(NP), dma(6), dma(6), dma(6), dma(3), dma(1),
            ],
            compiler_params=pltpu.CompilerParams(
                collective_id=0, has_side_effects=True, vmem_limit_bytes=47 * 2**20),
        )(local_l.reshape(96, 8, 1536))
        return got.reshape(HW, 1536)

    return jax.shard_map(body, mesh=mesh, in_specs=(spec,), out_specs=spec, check_vma=False)
```

```python
import functools

import jax
import jax.numpy as jnp
from jax import lax
from jax.experimental import pallas as pl
from jax.experimental.pallas import tpu as pltpu
from jax.sharding import PartitionSpec as P

MESH = pl.DeviceIdType.MESH
F32 = jnp.float32

OFF_A = [(i, j) for i in range(1, 6) for j in range(i)]
OFF_B = [(i + 6, j + 6) for i in range(1, 6) for j in range(i)]
TILES = OFF_A + OFF_B
TIDX = {ij: t for t, ij in enumerate(TILES)}
CHUNKS = [None, (0, 6), (6, 10), (10, 15), None, (15, 21), (21, 25), (25, 30)]
NC = len(CHUNKS)
YONLY = (1, 2, 3)
NF, NG, ND, SIB = range(4)
CP = [(0, 0, 8), (1, 0, 8), (2, 0, 8), (3, 0, 8), (4, 0, 8), (5, 0, 4), (5, 4, 8)]
NP = len(CP)
TG = [(0, 1), (2, 3), (4,), (5,), (6,)]
ORDER = [
    "g0 f0 c1 f2", "f1 f4 F0 c0", "f5 F2 f7 g5", "D0 G0 R0 I0", "F1 Q0 f3 R1", "E1 g4 F4 c5",
    "A1 E2 C0 F5", "F3 A2 E3 C1", "G5 R2 A3 f6", "E4 G4 c4 g6", "D4 C2 R3 C3", "A4 V0 E5 F6",
    "V1 c3 D5 R4", "G6 I1 A5 T0", "Q1 S0 C4 V2", "c2 R5 B1 D6", "V3 B2 P0 F7", "g7 T1 X0 B3",
    "Y0 R6 a0 C5", "V4 B4 X1 D7", "T2 G7 P1 X2", "c6 C6 V5 R7", "B5 T3 V6 X3", "T4 P2 X4 X5",
    "Y1 Y2 o0 Y4", "Y3 Y5",
]
MODES = [2, 1, 3, 3, 0, 2, 1, 3]
W, T2, JW, HW = 128, 256, 384, 768
QW, HALF, SH = 32, 64, 24
TWO, THREE, SIX = range(2), range(3), range(6)


def dot(a, b):
    return jnp.dot(a, b, precision=lax.Precision.HIGHEST, preferred_element_type=F32)


def kernel(l_hbm, out, lt, ld, raw, ea, c0, xa, xb, bx, tt, db, oa, xc, oc, zz, acc, accx, ys,
           loc, snd, rcv, crcv, trcv, orcv, brcv, bloc, misc_r, ercv, osem):
    row = lax.axis_index("row")
    y = lax.axis_index("col")
    x = row // 2
    k = row % 2
    ox, ok, oy = 1 - x, 1 - k, 1 - y
    sid = {"row": 2 * x + ok, "col": y}
    xid = {"row": 2 * ox + k, "col": y}
    yid = {"row": row, "col": oy}

    def way(c, core):
        return (core, 1 - core, 1, 0)[MODES[c]]

    def first(c):
        v = way(c, k)
        return {"row": row + (1 - v) * 2 * (1 - 2 * x), "col": y + v * (1 - 2 * y)}

    def second(c):
        v = 1 - way(c, k)
        return {"row": row + (1 - v) * 2 * (1 - 2 * x), "col": y + v * (1 - 2 * y)}

    def from_first(c, core):
        v = way(c, core)
        return y + v * (1 - 2 * y), x + (1 - v) * (1 - 2 * x)

    def from_second(c, core):
        v = 1 - way(c, core)
        return y + v * (1 - 2 * y), x + (1 - v) * (1 - 2 * x)

    started = []

    def remote(src, dst, ss, rs, dev):
        cp = pltpu.make_async_remote_copy(src_ref=src, dst_ref=dst, send_sem=ss, recv_sem=rs,
                                          device_id=dev, device_id_type=MESH)
        return cp

    def piece(c, q, p, xs):
        if CHUNKS[c] is None:
            return ld.at[c // 4, q, p, :, xs, :, :]
        a, b = CHUNKS[c]
        return lt.at[a:b, q, p, :, xs, :, :]

    def put(c, kind, q, xs, dev):
        ref = piece(c, q, k, xs)
        cp = remote(ref, ref, snd.at[0], rcv.at[c, kind], dev)
        cp.start()
        started.append(cp)

    def got(c, kind, q, p, xs):
        ref = piece(c, q, p, xs)
        remote(ref, ref, snd.at[0], rcv.at[c, kind], sid).wait_recv()

    def local_copies(c):
        if CHUNKS[c] is None:
            h = c // 4
            low, high = [], []
            for n in SIX:
                i = 6 * h + n
                cols = slice(W * i, W * i + W)
                low.append(pltpu.make_async_copy(l_hbm.at[8 * i:8 * i + 6, :, cols], raw.at[h, n], loc.at[c]))
                high.append(pltpu.make_async_copy(l_hbm.at[8 * i + 6:8 * i + 8, :, cols],
                                                  ld.at[h, y, k, 4 * n + 2:4 * n + 4, x, :, :], loc.at[c]))
            return low + high
        a, b = CHUNKS[c]
        return [pltpu.make_async_copy(l_hbm.at[8 * i:8 * i + 8, :, W * j:W * j + W],
                                      lt.at[a + n, y, k, :, x, :, :], loc.at[c])
                for n, (i, j) in enumerate(TILES[a:b])]

    barrier = pltpu.get_barrier_semaphore()
    for dev in (xid, yid, sid):
        pl.semaphore_signal(barrier, inc=1, device_id=dev, device_id_type=MESH)
    steps = [(name[0], int(name[1:] or 0)) for group in ORDER for name in group.split()]
    c0load = pltpu.make_async_copy(l_hbm.at[48:96, :, 0:HW], c0.at[y, k], loc.at[NC])
    loads = {}
    for what, n in steps:
        if what in "fg" and n not in loads:
            loads[n] = local_copies(n)
            for cp in loads[n]:
                cp.start()
        if what in "cC" and NC not in loads:
            c0load.start()
            loads[NC] = [c0load]
    pl.semaphore_wait(barrier, 3)

    lane = lax.broadcasted_iota(jnp.int32, (8, W), 1)
    grp = lane // 16

    def turn(v, by):
        return jnp.concatenate([v[:, by:], v[:, :by]], axis=1)

    def loaded(c):
        copies = loads.pop(c, [])
        for cp in copies:
            cp.wait()
        if copies and c < NC and CHUNKS[c] is None:
            h = c // 4
            for n in SIX:
                for e in TWO:
                    v = jnp.where(lane < W - QW, raw[h, n, 4 + e], turn(raw[h, n, e], QW))
                    ld[h, y, k, 4 * n + e, x] = v
            for g in THREE:
                for e in TWO:
                    v = jnp.where(lane < HALF, raw[h, 2 * g, 2 + e], turn(raw[h, 2 * g + 1, 2 + e], HALF))
                    ld[h, y, k, SH + 2 * g + e, x] = v

    def own_first(c):
        loaded(c)
        put(c, NF, y, x, yid if c in YONLY else first(c))
        put(c, SIB, y, x, sid)

    def own_second(c):
        loaded(c)
        put(c, NG, y, x, second(c))

    def cref(n, q, p):
        s, m0, m1 = CP[n]
        return c0.at[q, p, 8 * s + m0:8 * s + m1]

    def cput(n, kind, q, dev):
        ref = cref(n, q, k)
        return remote(ref, ref, snd.at[0], crcv.at[n, kind], dev)

    def cgot(n, kind, q, p):
        ref = cref(n, q, p)
        remote(ref, ref, snd.at[0], crcv.at[n, kind], sid).wait_recv()

    def clear():
        xa[...] = jnp.zeros(xa.shape, F32)
        xb[...] = jnp.zeros(xb.shape, F32)
        zz[...] = jnp.zeros(zz.shape, F32)

    def serve_f(c):
        if c in YONLY:
            got(c, NF, oy, k, x)
            put(c, SIB, oy, x, sid)
            return
        q, xs = from_first(c, k)
        got(c, NF, q, k, xs)
        put(c, ND, q, xs, second(c))
        put(c, SIB, q, xs, sid)

    def serve_g(c):
        q, xs = from_second(c, k)
        got(c, NG, q, k, xs)
        put(c, SIB, q, xs, sid)

    def serve_d(c):
        got(c, ND, oy, k, ox)
        put(c, SIB, oy, ox, sid)

    def ready(c):
        if CHUNKS[c] is None:
            ref = ld.at[c // 4, :, ok]
        else:
            lo, hi = CHUNKS[c]
            ref = lt.at[lo:hi, :, ok, :, x] if c in YONLY else lt.at[lo:hi, :, ok]
        remote(ref, ref, snd.at[0], rcv.at[c, SIB], sid).wait_recv()

    G6 = 3
    lane48 = lax.broadcasted_iota(jnp.int32, (8 * G6, W), 1)
    sub48 = lax.broadcasted_iota(jnp.int32, (8 * G6, W), 0) % 8
    base48 = (lane48 // 16) * 16
    def rowcast(v, e):
        v3 = v.reshape(G6, 8, W)[:, e:e + 1, :]
        return jnp.broadcast_to(v3, (G6, 8, W)).reshape(8 * G6, W)

    def dl(half, g, q, p, m, sg):
        at = 4 * (2 * g + k)
        if m >= 4:
            return ld[half, q, p, at + m - 4, sg]
        if m < 2:
            return turn(ld[half, q, p, at + m, sg], W - QW)
        v = ld[half, q, p, SH + 2 * g + m - 2, sg]
        return jnp.where(k == 1, turn(v, HALF), v)

    def substitute(half):
        sub = {}
        for p in TWO:
            for sg in TWO:
                for q in TWO:
                    rows = []
                    for g in range(G6):
                        v = jnp.zeros((8, W), F32)
                        for m in range(8):
                            v = jnp.where(grp == m, dl(half, g, q, p, m, sg), v)
                        rows.append(v)
                    sub[2 * sg + p, q] = jnp.concatenate(rows, axis=0)
        yv = {}
        for be in range(4):
            for q in TWO:
                if be % 2 == q:
                    yv[be, q] = jnp.where(lane48 % 16 == 8 * (be // 2) + sub48, 1.0, 0.0).astype(F32)
                else:
                    yv[be, q] = jnp.zeros((8 * G6, W), F32)

        for be in range(4):
            for e in range(8):
                idx = base48 + (8 * (be // 2) + e)
                gs = {b2: jnp.take_along_axis(sub[b2, be % 2], idx, axis=1, mode="promise_in_bounds")
                      for b2 in range(be, 4)}
                rinv = 1.0 / rowcast(gs[be], e)
                for q in TWO:
                    piv = rowcast(yv[be, q], e) * rinv
                    for b2 in range(be, 4):
                        new = yv[b2, q] - gs[b2] * piv
                        if b2 == be:
                            new = jnp.where(sub48 > e, new, jnp.where(sub48 == e, piv, yv[b2, q]))
                        yv[b2, q] = new
        for be in range(4):
            for q in TWO:
                ys[be, q] = yv[be, q].reshape(G6, 8, W)

    lane256 = lax.broadcasted_iota(jnp.int32, (8, T2), 1) % W

    def invert(half, count=G6):
        dd, ll = [], []
        for n in range(count):
            g = n
            rows = []
            for p in TWO:
                for m in range(8):
                    for sg in TWO:
                        parts = [jnp.where(grp == m, ys[2 * sg + p, q, g], 0.0) for q in TWO]
                        rows.append(jnp.concatenate(parts, axis=1))
            dd.append(rows)
            ll.append([jnp.concatenate([dl(half, g, q, p, m, sg) for q in TWO], axis=1)
                       for p in TWO for m in range(8) for sg in TWO])
        for h8 in (2, 4, 8):
            odd = [b for b in range(32) if (b % 16) // h8 % 2 == 1]
            zero = jnp.zeros((8, T2), F32)
            tds = []
            for n in range(count):
                mo = [jnp.where(lane256 // (8 * h8) == (b % 16) // h8 - 1, ll[n][b], 0.0) for b in odd]
                tds.append(dot(jnp.concatenate(mo, axis=0), jnp.concatenate(dd[n], axis=0)))
            for n in range(count):
                tfull = [zero] * 32
                for o, b in enumerate(odd):
                    tfull[b] = tds[n][8 * o:8 * o + 8]
                xo = dot(jnp.concatenate([dd[n][b] for b in odd], axis=0), jnp.concatenate(tfull, axis=0))
                for o, b in enumerate(odd):
                    dd[n][b] = dd[n][b] - xo[8 * o:8 * o + 8]
        for n in range(count):
            db[G6 * half + n, k] = jnp.concatenate(dd[n], axis=0)
        dbcopy(half, k).start()

    def dbcopy(half, kk):
        ref = db.at[G6 * half:G6 * half + G6, kk]
        return remote(ref, ref, snd.at[0], misc_r.at[half], sid)

    def ltile(t):
        return jnp.concatenate([lt[t, q].reshape(T2, W) for q in TWO], axis=1)

    need = [0, 1, 1, 0, 0, 1]

    def place_a(i):
        @pl.when(k == need[i])
        def _():
            t = i // 2
            d = db[i // 2, i % 2, :, pl.ds(pl.multiple_of(y * W, W), W)]
            xa[i, :, :, :, :, W * t:W * t + W] = d.reshape(2, 8, 2, 8, W)

    def ecopy(i, xs):
        n = W * ((i + 1) // 2)
        ref = ea.at[i, :, :, xs, :, 0:n]
        return remote(ref, ref, snd.at[0], ercv.at[i], xid)

    def sum_a(i):
        for j in range(i):
            n = W * (j // 2 + 1)
            lhs = jnp.concatenate([lt[TIDX[i, j], q, :, :, x].reshape(W, W) for q in TWO], axis=1)
            d = dot(lhs, xa[j, :, :, :, :, 0:n].reshape(T2, n))
            n0 = 0 if j == 0 else W * ((j - 1) // 2 + 1)
            if n0:
                acc[0:W, 0:n0] = acc[0:W, 0:n0] + d[:, 0:n0]
            if n > n0:
                acc[0:W, n0:n] = d[:, n0:n]
        n = W * ((i + 1) // 2)
        ea[i, :, :, x, :, 0:n] = acc[0:W, 0:n].reshape(2, 8, 8, n)
        ecopy(i, x).start()

    def step_a(i):
        ecopy(i, ox).wait_recv()
        n = W * ((i + 1) // 2)
        r = -dot(db[i // 2, i % 2], ea[i, :, :, :, :, 0:n].reshape(T2, n))
        xa[i, :, :, :, :, 0:n] = r.reshape(2, 8, 2, 8, n)
        place_a(i)

    def place_b(i):
        d = db[3 + i // 2, i % 2, :, pl.ds(pl.multiple_of(k * W, W), W)]
        xb[i, :, :, :, :, W * i:W * i + W] = d.reshape(2, 8, 2, 8, W)

    def step_b(i):
        for j in range(i):
            n = W * (j + 1)
            d = dot(ltile(TIDX[i + 6, j + 6]), xb[j, :, :, :, :, 0:n].reshape(T2, n))
            if j:
                acc[:, 0:n - W] = acc[:, 0:n - W] + d[:, 0:n - W]
            acc[:, n - W:n] = d[:, n - W:n]
        n = W * i
        r = -dot(db[3 + i // 2, i % 2], acc[:, 0:n])
        xb[i, :, :, :, :, 0:n] = r.reshape(2, 8, 2, 8, n)
        place_b(i)

    outs = []

    def put_out(src, dst):
        cp = pltpu.make_async_copy(src, dst, osem.at[0])
        cp.start()
        outs.append(cp)

    def jcol(t, kk):
        return [kk, 3 - kk, 4 + kk][t]

    def lanes(t, kk):
        return pl.ds(pl.multiple_of(W * jcol(t, kk), W), W)

    oacopy = remote(xa.at[:, ok, :, x, :, :], oa, snd.at[0], misc_r.at[2], sid)

    def finish_a():
        oacopy.start()
        for i in SIX:
            put_out(zz, out.at[i, :, :, HW:2 * HW])
        for t in THREE:
            put_out(xa.at[:, k, :, x, :, W * t:W * t + W], out.at[0:6, :, :, lanes(t, k)])

    def finish_oa():
        remote(oa, oa, snd.at[0], misc_r.at[2], sid).wait_recv()
        for t in THREE:
            put_out(oa.at[:, :, :, W * t:W * t + W], out.at[0:6, :, :, lanes(t, ok)])

    def bxcopy(i, kk):
        return remote(xb.at[i, :, :, x, :, :], bx.at[kk, i], snd.at[0], brcv.at[i], sid)

    def bxlocal(i):
        return pltpu.make_async_copy(xb.at[i, :, :, x, :, :], bx.at[k, i], bloc.at[i])

    def send_b(i):
        bxcopy(i, k).start()
        bxlocal(i).start()

    def get_b(i):
        bxlocal(i).wait()
        bxcopy(i, ok).wait_recv()
        put_out(bx.at[y, i, k], out.at[6 + i, :, :, HW:2 * HW])

    def tcopy(n, xs):
        s, m0, m1 = CP[n]
        ref = tt.at[s, :, m0:m1, xs, :, :]
        return remote(ref, ref, snd.at[0], trcv.at[n], xid)

    def serve_c(n):
        cgot(n, 0, oy, k)
        cput(n, 1, oy, sid).start()

    def do_t(h):
        group = TG[h]
        for n in group:
            s, m0, m1 = CP[n]
            both = c0.at[:, ok, 8 * s + m0:8 * s + m1]
            remote(both, both, snd.at[0], crcv.at[n, 1], sid).wait_recv()
        lo = 8 * CP[group[0]][0] + CP[group[0]][1]
        hi = 8 * CP[group[-1]][0] + CP[group[-1]][2]
        g = 8 * (hi - lo)
        for u in THREE:
            w = W * (u + 1)
            parts = []
            for j in (2 * u, 2 * u + 1):
                for q in TWO:
                    parts.append(c0[q, :, lo:hi, :, W * j:W * j + W].reshape(2 * g, W))
            rhs = jnp.concatenate([xa[2 * u + e, :, :, :, :, 0:w].reshape(T2, w) for e in TWO], axis=0)
            d = dot(jnp.concatenate(parts, axis=1), rhs)
            if u:
                acc[0:2 * g, 0:w - W] = acc[0:2 * g, 0:w - W] + d[:, 0:w - W]
            acc[0:2 * g, w - W:w] = d[:, w - W:w]
        for n in group:
            s, m0, m1 = CP[n]
            at = 8 * (8 * s + m0 - lo)
            size = 8 * (m1 - m0)
            for p in TWO:
                r = acc[p * g + at:p * g + at + size, 0:JW]
                tt[s, p, m0:m1, x, :, :] = r.reshape(m1 - m0, 8, JW)
            tcopy(n, x).start()

    def tgot(s):
        for n in range(NP):
            if CP[n][0] == s:
                tcopy(n, ox).wait_recv()

    def bpart(s, count, u, nu):
        parts = []
        for e in range(nu):
            ln = pl.ds(pl.multiple_of((u + e) * W, W), W)
            for q in TWO:
                parts.append(bx[q, s:s + count, :, :, :, ln].reshape(count * W, W))
        rhs = jnp.concatenate([tt[u + e].reshape(T2, JW) for e in range(nu)], axis=0)
        return dot(jnp.concatenate(parts, axis=1), rhs)

    def do_p(a):
        for s in (2 * a, 2 * a + 1):
            get_b(s)

        def body(it, carry):
            accx[...] = accx[...] - bpart(2 * a, 2, 2 * it, 2)
            return carry

        if a > 1:
            accx[...] = jnp.zeros((T2, JW), F32)
            lax.fori_loop(0, a, body, 0)
        elif a == 1:
            accx[...] = -bpart(2, 2, 0, 2)

    def do_x(s):
        tgot(s)
        if s == 0:
            accx[...] = -bpart(0, 2, 0, 1)
        elif s % 2 == 0:
            accx[...] = accx[...] - bpart(s, 2, s, 1)
        else:
            accx[W:, :] = accx[W:, :] - bpart(s, 1, s, 1)
        at = W * (s % 2)
        xc[s] = accx[at:at + W, :].reshape(2, 8, 8, JW)
        remote(xc.at[s, ok], oc.at[s], snd.at[0], orcv.at[s], sid).start()
        for t in THREE:
            put_out(xc.at[s, k, :, :, W * t:W * t + W], out.at[6 + s, :, :, lanes(t, k)])

    def finish_x(s):
        remote(oc.at[s], oc.at[s], snd.at[0], orcv.at[s], sid).wait_recv()
        for t in THREE:
            put_out(oc.at[s, :, :, W * t:W * t + W], out.at[6 + s, :, :, lanes(t, ok)])

    def inv(half):
        substitute(half)
        invert(half)

    def get_d(half):
        dbcopy(half, ok).wait_recv()
        (place_b if half else place_a)(0)

    def do_b(i):
        step_b(i)
        send_b(i)

    def csend(n):
        loaded(NC)
        cput(n, 0, y, yid).start()

    def csib(n):
        loaded(NC)
        cput(n, 1, y, sid).start()

    run = {"f": own_first, "g": own_second, "F": serve_f, "G": serve_g, "D": serve_d, "R": ready, "I": inv,
           "Q": get_d, "A": step_a, "E": sum_a, "B": do_b, "S": send_b, "C": csend, "c": csib, "V": serve_c, "T": do_t,
           "X": do_x, "P": do_p, "Y": finish_x, "a": lambda _: finish_a(), "o": lambda _: finish_oa()}
    cleared = False
    for what, n in steps:
        if what in "FGDR" and not cleared:
            clear()
            cleared = True
        with jax.named_scope(f"{what}{n}"):
            run[what](n)

    for cp in started:
        cp.wait_send()
    for n in range(NP):
        cput(n, 0, y, yid).wait_send()
        cput(n, 1, y, sid).wait_send()
        cput(n, 1, oy, sid).wait_send()
        tcopy(n, x).wait_send()
    for s in SIX:
        bxcopy(s, k).wait_send()
        remote(xc.at[s, ok], oc.at[s], snd.at[0], orcv.at[s], sid).wait_send()
    for i in range(1, 6):
        ecopy(i, x).wait_send()
    dbcopy(0, k).wait_send()
    dbcopy(1, k).wait_send()
    oacopy.wait_send()
    for cp in outs:
        cp.wait()


def solution(mesh):
    spec = P(("batch", "row"), "col")
    vm = lambda *shape: pltpu.VMEM(shape, F32)
    dma = lambda *shape: pltpu.SemaphoreType.DMA(shape)

    def body(local_l):
        got = pl.pallas_call(
            kernel,
            name="tri_inverse",
            out_shape=jax.ShapeDtypeStruct((12, 8, 8, 1536), F32),
            in_specs=[pl.BlockSpec(memory_space=pl.ANY)],
            out_specs=pl.BlockSpec(memory_space=pl.ANY),
            scratch_shapes=[
                vm(30, 2, 2, 8, 2, 8, W),
                vm(2, 2, 2, 30, 2, 8, W),
                vm(2, 6, 6, 8, W),
                vm(6, 2, 8, 2, 8, JW),
                vm(2, 2, 48, 8, HW),
                vm(6, 2, 8, 2, 8, JW),
                vm(6, 2, 8, 2, 8, HW),
                vm(2, 6, 2, 8, 8, HW),
                vm(6, 2, 8, 2, 8, JW),
                vm(6, 2, T2, T2),
                vm(6, 8, 8, JW),
                vm(6, 2, 8, 8, JW),
                vm(6, 8, 8, JW),
                vm(8, 8, HW),
                vm(T2, HW),
                vm(T2, JW),
                vm(4, 2, 3, 8, W),
                dma(NC + 1), dma(1), dma(NC, 4), dma(NP, 2), dma(NP), dma(6), dma(6), dma(6), dma(3), dma(6), dma(1),
            ],
            compiler_params=pltpu.CompilerParams(
                collective_id=0, has_side_effects=True, vmem_limit_bytes=47 * 2**20),
        )(local_l.reshape(96, 8, 1536))
        return got.reshape(HW, 1536)

    return jax.shard_map(body, mesh=mesh, in_specs=(spec,), out_specs=spec, check_vma=False)
```

```python
import functools

import jax
import jax.numpy as jnp
from jax import lax
from jax.experimental import pallas as pl
from jax.experimental.pallas import tpu as pltpu
from jax.sharding import PartitionSpec as P

MESH = pl.DeviceIdType.MESH
F32 = jnp.float32

OFF_A = [(i, j) for i in range(1, 6) for j in range(i)]
OFF_B = [(i + 6, j + 6) for i in range(1, 6) for j in range(i)]
TILES = OFF_A + OFF_B
TIDX = {ij: t for t, ij in enumerate(TILES)}
CHUNKS = [None, (0, 6), (6, 10), (10, 15), None, (15, 21), (21, 25), (25, 30)]
NC = len(CHUNKS)
YONLY = (1, 2, 3)
NF, NG, ND, SIB = range(4)
CP = [(0, 0, 8), (1, 0, 8), (2, 0, 8), (3, 0, 8), (4, 0, 8), (5, 0, 4), (5, 4, 8)]
NP = len(CP)
TG = [(0, 1), (2, 3), (4,), (5,), (6,)]
ORDER = [
    "g0 f0 f1 f3", "f4 G0 c0 F0", "D0 g5 R0 f7", "f2 I0 F1 f5", "Q0 g4 C0 C1", "c2 F3 R1 E1",
    "R3 F4 F2 A1", "E2 R2 F5 A2", "E3 A3 c5 f6", "E4 c1 C2 g6", "G4 G5 V0 D4", "D5 A4 E5 C3",
    "V1 R5 F6 R4", "c3 c4 g7 I1", "V2 A5 T0 C4", "G6 V3 Q1 S0", "D6 B1 T1 c6", "B2 R6 a0 B3",
    "C5 G7 V4 F7", "B4 P0 X0 X1", "V5 T2 C6 P1", "D7 Y0 T3 o0", "X2 V6 R7 B5", "X3 T4 P2 X4",
    "X5 Y4 Y1 Y3", "Y2 Y5",
]
MODES = [2, 2, 0, 3, 1, 2, 1, 3]
W, T2, JW, HW = 128, 256, 384, 768
QW, HALF, SH = 32, 64, 24
TWO, THREE, SIX = range(2), range(3), range(6)


def dot(a, b):
    return jnp.dot(a, b, precision=lax.Precision.HIGHEST, preferred_element_type=F32)


def kernel(l_hbm, out, lt, ld, raw, ea, c0, xa, xb, bx, tt, db, oa, xc, oc, zz, acc, accx, ys,
           loc, snd, rcv, crcv, trcv, orcv, brcv, bloc, misc_r, ercv, osem):
    row = lax.axis_index("row")
    y = lax.axis_index("col")
    x = row // 2
    k = row % 2
    ox, ok, oy = 1 - x, 1 - k, 1 - y
    sid = {"row": 2 * x + ok, "col": y}
    xid = {"row": 2 * ox + k, "col": y}
    yid = {"row": row, "col": oy}

    def way(c, core):
        return (core, 1 - core, 1, 0)[MODES[c]]

    def first(c):
        v = way(c, k)
        return {"row": row + (1 - v) * 2 * (1 - 2 * x), "col": y + v * (1 - 2 * y)}

    def second(c):
        v = 1 - way(c, k)
        return {"row": row + (1 - v) * 2 * (1 - 2 * x), "col": y + v * (1 - 2 * y)}

    def from_first(c, core):
        v = way(c, core)
        return y + v * (1 - 2 * y), x + (1 - v) * (1 - 2 * x)

    def from_second(c, core):
        v = 1 - way(c, core)
        return y + v * (1 - 2 * y), x + (1 - v) * (1 - 2 * x)

    started = []

    def remote(src, dst, ss, rs, dev):
        cp = pltpu.make_async_remote_copy(src_ref=src, dst_ref=dst, send_sem=ss, recv_sem=rs,
                                          device_id=dev, device_id_type=MESH)
        return cp

    def piece(c, q, p, xs):
        if CHUNKS[c] is None:
            return ld.at[c // 4, q, p, :, xs, :, :]
        a, b = CHUNKS[c]
        return lt.at[a:b, q, p, :, xs, :, :]

    def put(c, kind, q, xs, dev):
        ref = piece(c, q, k, xs)
        cp = remote(ref, ref, snd.at[0], rcv.at[c, kind], dev)
        cp.start()
        started.append(cp)

    def got(c, kind, q, p, xs):
        ref = piece(c, q, p, xs)
        remote(ref, ref, snd.at[0], rcv.at[c, kind], sid).wait_recv()

    def local_copies(c):
        if CHUNKS[c] is None:
            h = c // 4
            low, high = [], []
            for n in SIX:
                i = 6 * h + n
                cols = slice(W * i, W * i + W)
                low.append(pltpu.make_async_copy(l_hbm.at[8 * i:8 * i + 6, :, cols], raw.at[h, n], loc.at[c]))
                high.append(pltpu.make_async_copy(l_hbm.at[8 * i + 6:8 * i + 8, :, cols],
                                                  ld.at[h, y, k, 4 * n + 2:4 * n + 4, x, :, :], loc.at[c]))
            return low + high
        a, b = CHUNKS[c]
        return [pltpu.make_async_copy(l_hbm.at[8 * i:8 * i + 8, :, W * j:W * j + W],
                                      lt.at[a + n, y, k, :, x, :, :], loc.at[c])
                for n, (i, j) in enumerate(TILES[a:b])]

    barrier = pltpu.get_barrier_semaphore()
    for dev in (xid, yid, sid):
        pl.semaphore_signal(barrier, inc=1, device_id=dev, device_id_type=MESH)
    steps = [(name[0], int(name[1:] or 0)) for group in ORDER for name in group.split()]
    c0load = pltpu.make_async_copy(l_hbm.at[48:96, :, 0:HW], c0.at[y, k], loc.at[NC])
    loads = {}
    for what, n in steps:
        if what in "fg" and n not in loads:
            loads[n] = local_copies(n)
            for cp in loads[n]:
                cp.start()
        if what in "cC" and NC not in loads:
            c0load.start()
            loads[NC] = [c0load]
    pl.semaphore_wait(barrier, 3)

    lane = lax.broadcasted_iota(jnp.int32, (8, W), 1)
    grp = lane // 16

    def turn(v, by):
        return jnp.concatenate([v[:, by:], v[:, :by]], axis=1)

    def loaded(c):
        copies = loads.pop(c, [])
        for cp in copies:
            cp.wait()
        if copies and c < NC and CHUNKS[c] is None:
            h = c // 4
            for n in SIX:
                for e in TWO:
                    v = jnp.where(lane < W - QW, raw[h, n, 4 + e], turn(raw[h, n, e], QW))
                    ld[h, y, k, 4 * n + e, x] = v
            for g in THREE:
                for e in TWO:
                    v = jnp.where(lane < HALF, raw[h, 2 * g, 2 + e], turn(raw[h, 2 * g + 1, 2 + e], HALF))
                    ld[h, y, k, SH + 2 * g + e, x] = v

    def own_first(c):
        loaded(c)
        put(c, NF, y, x, yid if c in YONLY else first(c))
        put(c, SIB, y, x, sid)

    def own_second(c):
        loaded(c)
        put(c, NG, y, x, second(c))

    def cref(n, q, p):
        s, m0, m1 = CP[n]
        return c0.at[q, p, 8 * s + m0:8 * s + m1]

    def cput(n, kind, q, dev):
        ref = cref(n, q, k)
        return remote(ref, ref, snd.at[0], crcv.at[n, kind], dev)

    def cgot(n, kind, q, p):
        ref = cref(n, q, p)
        remote(ref, ref, snd.at[0], crcv.at[n, kind], sid).wait_recv()

    def clear():
        xa[...] = jnp.zeros(xa.shape, F32)
        xb[...] = jnp.zeros(xb.shape, F32)
        zz[...] = jnp.zeros(zz.shape, F32)

    def serve_f(c):
        if c in YONLY:
            got(c, NF, oy, k, x)
            put(c, SIB, oy, x, sid)
            return
        q, xs = from_first(c, k)
        got(c, NF, q, k, xs)
        put(c, ND, q, xs, second(c))
        put(c, SIB, q, xs, sid)

    def serve_g(c):
        q, xs = from_second(c, k)
        got(c, NG, q, k, xs)
        put(c, SIB, q, xs, sid)

    def serve_d(c):
        got(c, ND, oy, k, ox)
        put(c, SIB, oy, ox, sid)

    def ready(c):
        if CHUNKS[c] is None:
            ref = ld.at[c // 4, :, ok]
        else:
            lo, hi = CHUNKS[c]
            ref = lt.at[lo:hi, :, ok, :, x] if c in YONLY else lt.at[lo:hi, :, ok]
        remote(ref, ref, snd.at[0], rcv.at[c, SIB], sid).wait_recv()

    G6 = 3
    lane48 = lax.broadcasted_iota(jnp.int32, (8 * G6, W), 1)
    sub48 = lax.broadcasted_iota(jnp.int32, (8 * G6, W), 0) % 8
    base48 = (lane48 // 16) * 16
    def rowcast(v, e):
        v3 = v.reshape(G6, 8, W)[:, e:e + 1, :]
        return jnp.broadcast_to(v3, (G6, 8, W)).reshape(8 * G6, W)

    def dl(half, g, q, p, m, sg):
        at = 4 * (2 * g + k)
        if m >= 4:
            return ld[half, q, p, at + m - 4, sg]
        if m < 2:
            return turn(ld[half, q, p, at + m, sg], W - QW)
        v = ld[half, q, p, SH + 2 * g + m - 2, sg]
        return jnp.where(k == 1, turn(v, HALF), v)

    def substitute(half):
        sub = {}
        for p in TWO:
            for sg in TWO:
                for q in TWO:
                    rows = []
                    for g in range(G6):
                        v = jnp.zeros((8, W), F32)
                        for m in range(8):
                            v = jnp.where(grp == m, dl(half, g, q, p, m, sg), v)
                        rows.append(v)
                    sub[2 * sg + p, q] = jnp.concatenate(rows, axis=0)
        yv = {}
        for be in range(4):
            for q in TWO:
                if be % 2 == q:
                    yv[be, q] = jnp.where(lane48 % 16 == 8 * (be // 2) + sub48, 1.0, 0.0).astype(F32)
                else:
                    yv[be, q] = jnp.zeros((8 * G6, W), F32)

        for be in range(4):
            for e in range(8):
                idx = base48 + (8 * (be // 2) + e)
                gs = {b2: jnp.take_along_axis(sub[b2, be % 2], idx, axis=1, mode="promise_in_bounds")
                      for b2 in range(be, 4)}
                rinv = 1.0 / rowcast(gs[be], e)
                for q in TWO:
                    piv = rowcast(yv[be, q], e) * rinv
                    for b2 in range(be, 4):
                        new = yv[b2, q] - gs[b2] * piv
                        if b2 == be:
                            new = jnp.where(sub48 > e, new, jnp.where(sub48 == e, piv, yv[b2, q]))
                        yv[b2, q] = new
        for be in range(4):
            for q in TWO:
                ys[be, q] = yv[be, q].reshape(G6, 8, W)

    lane256 = lax.broadcasted_iota(jnp.int32, (8, T2), 1) % W

    def invert(half, count=G6):
        dd, ll = [], []
        for n in range(count):
            g = n
            rows = []
            for p in TWO:
                for m in range(8):
                    for sg in TWO:
                        parts = [jnp.where(grp == m, ys[2 * sg + p, q, g], 0.0) for q in TWO]
                        rows.append(jnp.concatenate(parts, axis=1))
            dd.append(rows)
            ll.append([jnp.concatenate([dl(half, g, q, p, m, sg) for q in TWO], axis=1)
                       for p in TWO for m in range(8) for sg in TWO])
        for h8 in (2, 4, 8):
            odd = [b for b in range(32) if (b % 16) // h8 % 2 == 1]
            zero = jnp.zeros((8, T2), F32)
            tds = []
            for n in range(count):
                mo = [jnp.where(lane256 // (8 * h8) == (b % 16) // h8 - 1, ll[n][b], 0.0) for b in odd]
                tds.append(dot(jnp.concatenate(mo, axis=0), jnp.concatenate(dd[n], axis=0)))
            for n in range(count):
                tfull = [zero] * 32
                for o, b in enumerate(odd):
                    tfull[b] = tds[n][8 * o:8 * o + 8]
                xo = dot(jnp.concatenate([dd[n][b] for b in odd], axis=0), jnp.concatenate(tfull, axis=0))
                for o, b in enumerate(odd):
                    dd[n][b] = dd[n][b] - xo[8 * o:8 * o + 8]
        for n in range(count):
            db[G6 * half + n, k] = jnp.concatenate(dd[n], axis=0)
        dbcopy(half, k).start()

    def dbcopy(half, kk):
        ref = db.at[G6 * half:G6 * half + G6, kk]
        return remote(ref, ref, snd.at[0], misc_r.at[half], sid)

    def ltile(t):
        return jnp.concatenate([lt[t, q].reshape(T2, W) for q in TWO], axis=1)

    need = [0, 1, 1, 0, 0, 1]

    def place_a(i):
        @pl.when(k == need[i])
        def _():
            t = i // 2
            d = db[i // 2, i % 2, :, pl.ds(pl.multiple_of(y * W, W), W)]
            xa[i, :, :, :, :, W * t:W * t + W] = d.reshape(2, 8, 2, 8, W)

    def ecopy(i, xs):
        n = W * ((i + 1) // 2)
        ref = ea.at[i, :, :, xs, :, 0:n]
        return remote(ref, ref, snd.at[0], ercv.at[i], xid)

    def sum_a(i):
        for j in range(i):
            n = W * (j // 2 + 1)
            lhs = jnp.concatenate([lt[TIDX[i, j], q, :, :, x].reshape(W, W) for q in TWO], axis=1)
            d = dot(lhs, xa[j, :, :, :, :, 0:n].reshape(T2, n))
            n0 = 0 if j == 0 else W * ((j - 1) // 2 + 1)
            if n0:
                acc[0:W, 0:n0] = acc[0:W, 0:n0] + d[:, 0:n0]
            if n > n0:
                acc[0:W, n0:n] = d[:, n0:n]
        n = W * ((i + 1) // 2)
        ea[i, :, :, x, :, 0:n] = acc[0:W, 0:n].reshape(2, 8, 8, n)
        ecopy(i, x).start()

    def step_a(i):
        ecopy(i, ox).wait_recv()
        n = W * ((i + 1) // 2)
        r = -dot(db[i // 2, i % 2], ea[i, :, :, :, :, 0:n].reshape(T2, n))
        xa[i, :, :, :, :, 0:n] = r.reshape(2, 8, 2, 8, n)
        place_a(i)

    def place_b(i):
        d = db[3 + i // 2, i % 2, :, pl.ds(pl.multiple_of(k * W, W), W)]
        xb[i, :, :, :, :, W * i:W * i + W] = d.reshape(2, 8, 2, 8, W)

    def step_b(i):
        for j in range(i):
            n = W * (j + 1)
            d = dot(ltile(TIDX[i + 6, j + 6]), xb[j, :, :, :, :, 0:n].reshape(T2, n))
            if j:
                acc[:, 0:n - W] = acc[:, 0:n - W] + d[:, 0:n - W]
            acc[:, n - W:n] = d[:, n - W:n]
        n = W * i
        r = -dot(db[3 + i // 2, i % 2], acc[:, 0:n])
        xb[i, :, :, :, :, 0:n] = r.reshape(2, 8, 2, 8, n)
        place_b(i)

    outs = []

    def put_out(src, dst):
        cp = pltpu.make_async_copy(src, dst, osem.at[0])
        cp.start()
        outs.append(cp)

    def jcol(t, kk):
        return [kk, 3 - kk, 4 + kk][t]

    def lanes(t, kk):
        return pl.ds(pl.multiple_of(W * jcol(t, kk), W), W)

    oacopy = remote(xa.at[:, ok, :, x, :, :], oa, snd.at[0], misc_r.at[2], sid)

    def finish_a():
        oacopy.start()
        for i in SIX:
            put_out(zz, out.at[i, :, :, HW:2 * HW])
        for t in THREE:
            put_out(xa.at[:, k, :, x, :, W * t:W * t + W], out.at[0:6, :, :, lanes(t, k)])

    def finish_oa():
        remote(oa, oa, snd.at[0], misc_r.at[2], sid).wait_recv()
        for t in THREE:
            put_out(oa.at[:, :, :, W * t:W * t + W], out.at[0:6, :, :, lanes(t, ok)])

    def bxcopy(i, kk):
        return remote(xb.at[i, :, :, x, :, :], bx.at[kk, i], snd.at[0], brcv.at[i], sid)

    def bxlocal(i):
        return pltpu.make_async_copy(xb.at[i, :, :, x, :, :], bx.at[k, i], bloc.at[i])

    def send_b(i):
        bxcopy(i, k).start()
        bxlocal(i).start()

    def get_b(i):
        bxlocal(i).wait()
        bxcopy(i, ok).wait_recv()
        put_out(bx.at[y, i, k], out.at[6 + i, :, :, HW:2 * HW])

    def tcopy(n, xs):
        s, m0, m1 = CP[n]
        ref = tt.at[s, :, m0:m1, xs, :, :]
        return remote(ref, ref, snd.at[0], trcv.at[n], xid)

    def serve_c(n):
        cgot(n, 0, oy, k)
        cput(n, 1, oy, sid).start()

    def do_t(h):
        group = TG[h]
        for n in group:
            s, m0, m1 = CP[n]
            both = c0.at[:, ok, 8 * s + m0:8 * s + m1]
            remote(both, both, snd.at[0], crcv.at[n, 1], sid).wait_recv()
        lo = 8 * CP[group[0]][0] + CP[group[0]][1]
        hi = 8 * CP[group[-1]][0] + CP[group[-1]][2]
        g = 8 * (hi - lo)
        for u in THREE:
            w = W * (u + 1)
            parts = []
            for j in (2 * u, 2 * u + 1):
                for q in TWO:
                    parts.append(c0[q, :, lo:hi, :, W * j:W * j + W].reshape(2 * g, W))
            rhs = jnp.concatenate([xa[2 * u + e, :, :, :, :, 0:w].reshape(T2, w) for e in TWO], axis=0)
            d = dot(jnp.concatenate(parts, axis=1), rhs)
            if u:
                acc[0:2 * g, 0:w - W] = acc[0:2 * g, 0:w - W] + d[:, 0:w - W]
            acc[0:2 * g, w - W:w] = d[:, w - W:w]
        for n in group:
            s, m0, m1 = CP[n]
            at = 8 * (8 * s + m0 - lo)
            size = 8 * (m1 - m0)
            for p in TWO:
                r = acc[p * g + at:p * g + at + size, 0:JW]
                tt[s, p, m0:m1, x, :, :] = r.reshape(m1 - m0, 8, JW)
            tcopy(n, x).start()

    def tgot(s):
        for n in range(NP):
            if CP[n][0] == s:
                tcopy(n, ox).wait_recv()

    def bpart(s, count, u, nu):
        parts = []
        for e in range(nu):
            ln = pl.ds(pl.multiple_of((u + e) * W, W), W)
            for q in TWO:
                parts.append(bx[q, s:s + count, :, :, :, ln].reshape(count * W, W))
        rhs = jnp.concatenate([tt[u + e].reshape(T2, JW) for e in range(nu)], axis=0)
        return dot(jnp.concatenate(parts, axis=1), rhs)

    def do_p(a):
        for s in (2 * a, 2 * a + 1):
            get_b(s)

        def body(it, carry):
            accx[...] = accx[...] - bpart(2 * a, 2, 2 * it, 2)
            return carry

        if a > 1:
            accx[...] = jnp.zeros((T2, JW), F32)
            lax.fori_loop(0, a, body, 0)
        elif a == 1:
            accx[...] = -bpart(2, 2, 0, 2)

    def do_x(s):
        tgot(s)
        if s == 0:
            accx[...] = -bpart(0, 2, 0, 1)
        elif s % 2 == 0:
            accx[...] = accx[...] - bpart(s, 2, s, 1)
        else:
            accx[W:, :] = accx[W:, :] - bpart(s, 1, s, 1)
        at = W * (s % 2)
        xc[s] = accx[at:at + W, :].reshape(2, 8, 8, JW)
        remote(xc.at[s, ok], oc.at[s], snd.at[0], orcv.at[s], sid).start()
        for t in THREE:
            put_out(xc.at[s, k, :, :, W * t:W * t + W], out.at[6 + s, :, :, lanes(t, k)])

    def finish_x(s):
        remote(oc.at[s], oc.at[s], snd.at[0], orcv.at[s], sid).wait_recv()
        for t in THREE:
            put_out(oc.at[s, :, :, W * t:W * t + W], out.at[6 + s, :, :, lanes(t, ok)])

    def inv(half):
        substitute(half)
        invert(half)

    def get_d(half):
        dbcopy(half, ok).wait_recv()
        (place_b if half else place_a)(0)

    def do_b(i):
        step_b(i)
        send_b(i)

    def csend(n):
        loaded(NC)
        cput(n, 0, y, yid).start()

    def csib(n):
        loaded(NC)
        cput(n, 1, y, sid).start()

    run = {"f": own_first, "g": own_second, "F": serve_f, "G": serve_g, "D": serve_d, "R": ready, "I": inv,
           "Q": get_d, "A": step_a, "E": sum_a, "B": do_b, "S": send_b, "C": csend, "c": csib, "V": serve_c, "T": do_t,
           "X": do_x, "P": do_p, "Y": finish_x, "a": lambda _: finish_a(), "o": lambda _: finish_oa()}
    cleared = False
    for what, n in steps:
        if what in "FGDR" and not cleared:
            clear()
            cleared = True
        with jax.named_scope(f"{what}{n}"):
            run[what](n)

    for cp in started:
        cp.wait_send()
    for n in range(NP):
        cput(n, 0, y, yid).wait_send()
        cput(n, 1, y, sid).wait_send()
        cput(n, 1, oy, sid).wait_send()
        tcopy(n, x).wait_send()
    for s in SIX:
        bxcopy(s, k).wait_send()
        remote(xc.at[s, ok], oc.at[s], snd.at[0], orcv.at[s], sid).wait_send()
    for i in range(1, 6):
        ecopy(i, x).wait_send()
    dbcopy(0, k).wait_send()
    dbcopy(1, k).wait_send()
    oacopy.wait_send()
    for cp in outs:
        cp.wait()


def solution(mesh):
    spec = P(("batch", "row"), "col")
    vm = lambda *shape: pltpu.VMEM(shape, F32)
    dma = lambda *shape: pltpu.SemaphoreType.DMA(shape)

    def body(local_l):
        got = pl.pallas_call(
            kernel,
            name="tri_inverse",
            out_shape=jax.ShapeDtypeStruct((12, 8, 8, 1536), F32),
            in_specs=[pl.BlockSpec(memory_space=pl.ANY)],
            out_specs=pl.BlockSpec(memory_space=pl.ANY),
            scratch_shapes=[
                vm(30, 2, 2, 8, 2, 8, W),
                vm(2, 2, 2, 30, 2, 8, W),
                vm(2, 6, 6, 8, W),
                vm(6, 2, 8, 2, 8, JW),
                vm(2, 2, 48, 8, HW),
                vm(6, 2, 8, 2, 8, JW),
                vm(6, 2, 8, 2, 8, HW),
                vm(2, 6, 2, 8, 8, HW),
                vm(6, 2, 8, 2, 8, JW),
                vm(6, 2, T2, T2),
                vm(6, 8, 8, JW),
                vm(6, 2, 8, 8, JW),
                vm(6, 8, 8, JW),
                vm(8, 8, HW),
                vm(T2, HW),
                vm(T2, JW),
                vm(4, 2, 3, 8, W),
                dma(NC + 1), dma(1), dma(NC, 4), dma(NP, 2), dma(NP), dma(6), dma(6), dma(6), dma(3), dma(6), dma(1),
            ],
            compiler_params=pltpu.CompilerParams(
                collective_id=0, has_side_effects=True, vmem_limit_bytes=47 * 2**20),
        )(local_l.reshape(96, 8, 1536))
        return got.reshape(HW, 1536)

    return jax.shard_map(body, mesh=mesh, in_specs=(spec,), out_specs=spec, check_vma=False)
```
